256 devices in a mesh: groups: 4 (over x, y), seq: 32 (over z), head: 2 (over core).
Axes of the slice: x: 2, y: 2, z: 32, core: 2. Of those that a mesh axis runs over, the one named last changes fastest.
The devices are a block of a 4x8x32 slice.
Arguments:
- queries: bfloat16 [16384, 28, 128], P(('groups', 'seq'), 'head'), parts along dimension 0, may hold values from -400 to 400, as said below
- request_image: int32 [16384, 1], P(('groups', 'seq')), parts along dimension 0, may hold values from 0 to 63; in each aligned block of 128 rows (0 to 127, 128 to 255, ...) at most 4 rows name the same one
- image_slot: int32 [256], P('groups'), parts along dimension 0, may hold values from 0 to 63, each once
- image_lengths: int32 [256], P(('groups', 'seq')), parts along dimension 0, may hold values from 640 to 1280
- image_keys: bfloat16 [256, 4, 1280, 128], P(('groups', 'seq'), 'head'), parts along dimension 0, may hold values from -6 to 6
- image_values: bfloat16 [256, 4, 1280, 128], P(('groups', 'seq'), 'head'), parts along dimension 0, may hold values from -6 to 6
- text_keys: bfloat16 [16384, 4, 64, 128], P(('groups', 'seq'), 'head'), parts along dimension 0, may hold values from -6 to 6
- text_values: bfloat16 [16384, 4, 64, 128], P(('groups', 'seq'), 'head'), parts along dimension 0, may hold values from -6 to 6
- text_lengths: int32 [16384], P(('groups', 'seq')), parts along dimension 0, may hold values from 1 to 64
Outputs:
- attention: bfloat16 [16384, 28, 128], P(('groups', 'seq'), 'head'), parts along dimension 0
The draws below stay inside these ranges and needn't reach their ends.
There are 4 independent parts, one for each index of `groups`. The reference program is written for one: setup_inputs(seed, part) draws one part's arguments, and reference() takes and returns one part's arrays. A program takes and returns all parts, laid end to end along the dimension named above; each array names one. Nothing has to cross between parts.
Inputs may be any that keep to these rules, and one draw needn't show every extreme that they name: queries are finite bfloat16 values. `request_image`: the requests of one index of seq name any one image at most 4 times, and in some index of seq some image is named exactly 4 times. `image_slot`: a permutation; the image in storage slot s is held by index s // 2 of seq.
All inputs are finite; a program needn't handle non-finite values.
Results may differ from the reference program's by a relative error of at most 0.0056.
Values may be sent and summed in bfloat16 or wider, within the bound.
A program may use at most 64 MiB of HBM per device.

```python
import math
import jax
import jax.numpy as jnp
import numpy as np
from jax import lax

D_HEAD = 128
KV_HEADS = 4
Q_HEADS = 28
IMG_TOK = 1280
TXT_TOK = 64
REQ_DEV = 128
REQUESTS = 4096
IMAGES = 64
MOST = 4


def draw_queries(key, part):
    base = jax.random.truncated_normal(key, -6.0, 6.0, (REQUESTS, Q_HEADS, D_HEAD), jnp.float32)
    return base.astype(jnp.bfloat16)


def touch_ends(drawn, own_key, smallest, high):
    spot = [jax.random.randint(jax.random.fold_in(own_key, axis), (), 0, length) for axis, length in enumerate(drawn.shape)]
    longest = drawn.shape.index(max(drawn.shape))
    neighbour = spot[:longest] + [(spot[longest] + 1) % drawn.shape[longest]] + spot[longest + 1:]
    return drawn.at[tuple(spot)].set(smallest).at[tuple(neighbour)].set(high)


def level_of(rng, extent, shards, smallest, largest):
    level, own = 1.0, jax.random.fold_in(rng, 6)
    for axis_at, shards_of in shards:
        steps = jnp.exp(jax.random.uniform(jax.random.fold_in(own, axis_at), (shards_of,), jnp.float32, smallest / len(shards), largest / len(shards)))
        level = level * jnp.repeat(steps, extent[axis_at] // shards_of).reshape([-1 if axis == axis_at else 1 for axis in range(len(extent))])
    return level


def routed_block(rng, own, number, rows, amount, top, limit, slope):
    ranking = jax.random.permutation(rng, amount)
    crowded, ordinary = portions_of(amount, rows * top, limit, slope, True), portions_of(amount, rows * top, limit, slope, False)
    places = jnp.arange(amount)

    def named(lengths, rotation):
        used = int((lengths > 0).sum())
        fixed = max(1, used // 4)
        passed = fixed + (places - fixed + rotation * (used - fixed)) % max(1, amount - fixed)
        return jnp.zeros((amount,), jnp.int32).at[ranking[jnp.where(places < fixed, places, passed)]].set(jnp.asarray(lengths, jnp.int32))

    lengths = jnp.where(number % 4 == 0, named(crowded, number // 4), named(ordinary, number - number // 4 - 1))
    mixed = jax.random.permutation(jax.random.fold_in(own, 3), amount)
    source_of, receiver = mixed[0:amount // 2 * 2:2], mixed[1:amount // 2 * 2:2]
    slack = jnp.minimum(lengths[source_of] - 1, limit - lengths[receiver]) // 2
    slack = jnp.where((source_of == ranking[0]) | (receiver == ranking[0]) | (lengths[receiver] == 0), 0, jnp.maximum(slack, 0))
    passed = jax.random.randint(jax.random.fold_in(own, 4), (amount // 2,), 0, 1 << 20) % (slack + 1)
    lengths = lengths.at[source_of].add(-passed).at[receiver].add(passed)
    members = jnp.searchsorted(jnp.cumsum(lengths), jnp.arange(rows * top), side="right").astype(jnp.int32)
    grid = members.reshape(top, rows).T
    grid = grid[jax.random.permutation(jax.random.fold_in(own, 1), rows)]
    rotation = jax.random.randint(jax.random.fold_in(own, 2), (rows, 1), 0, top)
    return jnp.take_along_axis(grid, (jnp.arange(top)[None, :] + rotation) % top, axis=1)


def portions_of(number_of, total, reach, slope, full):
    weights = [(1 << 20) // math.isqrt(grade ** slope) + 1 for grade in range(1, number_of + 1)]
    largest = reach if full else min(reach, max(-(-total // number_of), total * weights[0] // sum(weights)))
    least = 1 if total - largest >= number_of - 1 else 0
    given, spare = [largest] + [least] * (number_of - 1), total - largest - least * (number_of - 1)
    while spare > 0:
        candidates = [i for i in range(1, number_of) if given[i] < largest] or [i for i in range(1, number_of) if given[i] < reach]
        whole, remaining = sum([weights[i] for i in candidates]), spare
        for i in candidates:
            extra = min(reach - given[i], max(1, remaining * weights[i] // whole), spare)
            given[i] = given[i] + extra
            spare = spare - extra
    return np.array(given)


def scatter_about(key, extent, deviation, reach, split=(), held_as=jnp.bfloat16):
    result = deviation * jax.random.normal(key, extent, jnp.float32)
    if split:
        result = result * level_of(key, extent, split, -0.22, 0.18)
    return jnp.clip(result, -reach, reach).astype(held_as)


def setup_inputs(seed: int = 0, part: int = 0) -> dict:
    key_of = jax.random.split(jax.random.key(seed), 10)
    part_splits = jax.random.split(jax.random.fold_in(key_of[9], part), 10)
    queries = draw_queries(jax.random.fold_in(jax.random.fold_in(key_of[9], part), 71), part)
    request_image_keys = jax.random.split(jax.random.fold_in(part_splits[1], 1), REQUESTS // REQ_DEV)
    request_image_turns = jax.random.permutation(jax.random.fold_in(part_splits[1], 3), REQUESTS // REQ_DEV)
    request_image = jax.vmap(lambda own, number: routed_block(jax.random.fold_in(part_splits[1], 2), own, number, REQ_DEV, IMAGES, 1, MOST, 2))(request_image_keys, request_image_turns).reshape((REQUESTS, 1))
    image_slot = jax.random.permutation(part_splits[2], IMAGES).astype(jnp.int32)
    image_lengths = touch_ends(jax.random.randint(part_splits[3], (IMAGES,), IMG_TOK // 2, IMG_TOK + 1), jax.random.fold_in(part_splits[3], 1), IMG_TOK // 2, IMG_TOK).astype(jnp.int32)
    image_keys = scatter_about(part_splits[4], (IMAGES, KV_HEADS, IMG_TOK, D_HEAD), 1.0, 6.0, ((0, 32), (1, 2)))
    image_values = scatter_about(part_splits[5], (IMAGES, KV_HEADS, IMG_TOK, D_HEAD), 1.0, 6.0, ((0, 32), (1, 2)))
    text_keys = scatter_about(part_splits[6], (REQUESTS, KV_HEADS, TXT_TOK, D_HEAD), 1.0, 6.0, ((0, 32), (1, 2)))
    text_values = scatter_about(part_splits[7], (REQUESTS, KV_HEADS, TXT_TOK, D_HEAD), 1.0, 6.0, ((0, 32), (1, 2)))
    text_lengths = touch_ends(jax.random.randint(part_splits[8], (REQUESTS,), 1, TXT_TOK + 1), jax.random.fold_in(part_splits[8], 1), 1, TXT_TOK).astype(jnp.int32)
    return dict(queries=queries, request_image=request_image, image_slot=image_slot, image_lengths=image_lengths, image_keys=image_keys, image_values=image_values, text_keys=text_keys, text_values=text_values, text_lengths=text_lengths)


NEGATIVE = -1e+30

def partial_attend(query_heads, keys, values, valid, scale):
    scores = jnp.einsum('bhgd,bhtd->bhgt', query_heads, keys) * scale
    scores = jnp.where(valid, scores, NEGATIVE)
    highest = lax.optimization_barrier(jnp.max(scores, axis=-1, keepdims=True))
    weights = jnp.where(valid, jnp.exp(scores - highest), 0.0)
    total = lax.optimization_barrier(jnp.sum(weights, axis=-1, keepdims=True))
    rounded = lax.optimization_barrier(weights.astype(jnp.bfloat16)).astype(jnp.float32)
    output = jnp.einsum('bhgt,bhtd->bhgd', rounded, values) / total
    return (output, highest[..., 0] + jnp.log(total[..., 0]))

def merge_parts(image_out, image_lse, text_out, text_lse):
    highest = jnp.maximum(image_lse, text_lse)
    image_weight = jnp.exp(image_lse - highest)[..., None]
    text_weight = jnp.exp(text_lse - highest)[..., None]
    return (image_weight * image_out + text_weight * text_out) / (image_weight + text_weight)

def reference(queries, request_image, image_slot, image_lengths, image_keys, image_values, text_keys, text_values, text_lengths):
    scale = 1.0 / math.sqrt(D_HEAD)
    group = Q_HEADS // KV_HEADS
    slots = image_slot[request_image[:, 0]].astype(jnp.int32)
    blocks = REQUESTS // REQ_DEV

    def one_block(packed):
        block_queries, block_slots, block_tkeys, block_tvalues, block_tlen = packed
        query_heads = block_queries.astype(jnp.float32).reshape(REQ_DEV, KV_HEADS, group, D_HEAD)
        keys = image_keys[block_slots].astype(jnp.float32)
        values = image_values[block_slots].astype(jnp.float32)
        image_valid = (jnp.arange(IMG_TOK, dtype=jnp.int32)[None, :] < image_lengths[block_slots][:, None])[:, None, None, :]
        image_out, image_lse = partial_attend(query_heads, keys, values, image_valid, scale)
        image_out = lax.optimization_barrier(image_out.astype(jnp.bfloat16)).astype(jnp.float32)
        text_valid = (jnp.arange(TXT_TOK, dtype=jnp.int32)[None, :] < block_tlen[:, None])[:, None, None, :]
        text_out, text_lse = partial_attend(query_heads, block_tkeys.astype(jnp.float32), block_tvalues.astype(jnp.float32), text_valid, scale)
        merged = merge_parts(image_out, image_lse, text_out, text_lse)
        return merged.reshape(REQ_DEV, Q_HEADS, D_HEAD).astype(jnp.bfloat16)
    packed = (queries.reshape(blocks, REQ_DEV, Q_HEADS, D_HEAD), slots.reshape(blocks, REQ_DEV), text_keys.reshape(blocks, REQ_DEV, KV_HEADS, TXT_TOK, D_HEAD), text_values.reshape(blocks, REQ_DEV, KV_HEADS, TXT_TOK, D_HEAD), text_lengths.reshape(blocks, REQ_DEV))
    return lax.map(one_block, packed).reshape(REQUESTS, Q_HEADS, D_HEAD)
```

```python
import functools
import math

import jax
import jax.numpy as jnp
from jax import lax
from jax.experimental import pallas as pl
from jax.experimental.pallas import tpu as pltpu
from jax.sharding import PartitionSpec as P

NEGATIVE = -1e30
MESH = pl.DeviceIdType.MESH


def weigh(scores, valid):
    scores = jnp.where(valid, scores, NEGATIVE)
    highest = jnp.max(scores, axis=-1, keepdims=True)
    weights = jnp.where(valid, jnp.exp(scores - highest), 0.0)
    total = jnp.sum(weights, axis=-1, keepdims=True)
    return (weights.astype(jnp.bfloat16), total, highest)


def exchange_kernel(
    devices,
    most,
    scale,
    lengths_ref,
    asked_ref,
    keys_hbm,
    values_hbm,
    back_ref,
    back_lse_ref,
    keys,
    values,
    bias,
    incoming,
    answer,
    answer_lse,
    load_sem,
    ask_send,
    ask_recv,
    out_send,
    out_recv,
    lse_send,
    lse_recv,
):
    held, local_kv, tokens, _ = keys_hbm.shape
    slots = held * most
    group = asked_ref.shape[2] // slots
    me = lax.axis_index("seq")
    others = devices - 1

    def place(step):
        half = devices // 2 - (step + 1) // 2
        return half + (step % 2 == 0) * (devices - 2 * half)

    def ask(at):
        return pltpu.make_async_remote_copy(
            src_ref=asked_ref.at[at],
            dst_ref=incoming.at[at],
            send_sem=ask_send.at[at],
            recv_sem=ask_recv.at[at],
            device_id={"seq": (me + at) % devices},
            device_id_type=MESH,
        )

    def reply(at):
        target = {"seq": (me + devices - at) % devices}
        return (
            pltpu.make_async_remote_copy(
                src_ref=answer.at[at],
                dst_ref=back_ref.at[at],
                send_sem=out_send.at[at],
                recv_sem=out_recv.at[at],
                device_id=target,
                device_id_type=MESH,
            ),
            pltpu.make_async_remote_copy(
                src_ref=answer_lse.at[at],
                dst_ref=back_lse_ref.at[at],
                send_sem=lse_send.at[at],
                recv_sem=lse_recv.at[at],
                device_id=target,
                device_id_type=MESH,
            ),
        )

    loads = []
    for image in range(held):
        for head in range(local_kv):
            for number, (source, target) in enumerate(((keys_hbm, keys), (values_hbm, values))):
                loads.append(
                    pltpu.make_async_copy(
                        source.at[image, head],
                        target.at[head, pl.ds(image * tokens, tokens)],
                        load_sem.at[number, image, head],
                    )
                )
    for load in loads:
        load.start()

    barrier = pltpu.get_barrier_semaphore()

    def greet(step, carry):
        pl.semaphore_signal(
            barrier, inc=1, device_id={"seq": (me + 1 + step) % devices}, device_id_type=MESH
        )
        return carry

    lax.fori_loop(0, others, greet, 0)

    row = lax.broadcasted_iota(jnp.int32, (slots, held * tokens), 0)
    token = lax.broadcasted_iota(jnp.int32, (slots, held * tokens), 1)
    valid = jnp.zeros((slots, held * tokens), jnp.bool_)
    for image in range(held):
        mine = (row >= image * most) & (row < (image + 1) * most)
        inside = (token >= image * tokens) & (token < image * tokens + lengths_ref[image])
        valid = valid | (mine & inside)
    bias[...] = jnp.where(valid, 0.0, NEGATIVE)

    pl.semaphore_wait(barrier, others)

    def start_ask(step, carry):
        ask(place(step)).start()
        return carry

    lax.fori_loop(0, others, start_ask, 0)
    for load in loads:
        load.wait()

    lane = lax.broadcasted_iota(jnp.int32, (slots, 128), 1)
    line = lax.broadcasted_iota(jnp.int32, (slots, 128), 0)
    spot = lane - 16 * line

    def attend(read, at, out_to, lse_to):
        packed = jnp.zeros((slots, 128), jnp.float32)
        for head in range(local_kv):
            asked = read[at, head]
            scores = lax.dot_general(
                asked, keys[head], (((1,), (1,)), ((), ())), preferred_element_type=jnp.float32
            )
            scores = scores.reshape(group, slots, held * tokens) * scale + bias[...][None]
            highest = jnp.max(scores, axis=-1, keepdims=True)
            weights = jnp.exp(scores - highest)
            total = jnp.sum(weights, axis=-1, keepdims=True)
            weights = weights.astype(jnp.bfloat16).reshape(group * slots, held * tokens)
            mixed = jnp.dot(weights, values[head], preferred_element_type=jnp.float32)
            mixed = mixed / total.reshape(group * slots, 1)
            out_to[at, head] = mixed.astype(jnp.bfloat16)
            lse = highest + jnp.log(total)
            for member in range(group):
                packed = jnp.where(spot == head * group + member, lse[member], packed)
        lse_to[at] = jnp.sum(packed, axis=0, keepdims=True)

    attend(asked_ref, 0, back_ref, back_lse_ref)

    def serve(step, carry):
        @pl.when(step > 0)
        def _():
            for copy in reply(place(step - 1)):
                copy.start()

        at = place(step)
        ask(at).wait_recv()
        attend(incoming, at, answer, answer_lse)
        return carry

    lax.fori_loop(0, others, serve, 0)
    for copy in reply(place(others - 1)):
        copy.start()

    def finish(step, carry):
        at = place(step)
        ask(at).wait_send()
        for copy in reply(at):
            copy.wait()
        return carry

    lax.fori_loop(0, others, finish, 0)


def exchange(asked, keys, values, lengths, devices, most, scale):
    held, local_kv, tokens, size = keys.shape
    slots = held * most
    message = asked.shape[1:]
    vmem = pl.BlockSpec(memory_space=pltpu.VMEM)
    return pl.pallas_call(
        functools.partial(exchange_kernel, devices, most, scale),
        out_shape=(
            jax.ShapeDtypeStruct(asked.shape, jnp.bfloat16),
            jax.ShapeDtypeStruct((devices, 1, 128), jnp.float32),
        ),
        in_specs=[
            pl.BlockSpec(memory_space=pltpu.SMEM),
            vmem,
            pl.BlockSpec(memory_space=pl.ANY),
            pl.BlockSpec(memory_space=pl.ANY),
        ],
        out_specs=(vmem, vmem),
        scratch_shapes=[
            pltpu.VMEM((local_kv, held * tokens, size), jnp.bfloat16),
            pltpu.VMEM((local_kv, held * tokens, size), jnp.bfloat16),
            pltpu.VMEM((slots, held * tokens), jnp.float32),
            pltpu.VMEM((devices, *message), jnp.bfloat16),
            pltpu.VMEM((devices, *message), jnp.bfloat16),
            pltpu.VMEM((devices, 1, 128), jnp.float32),
            pltpu.SemaphoreType.DMA((2, held, local_kv)),
            pltpu.SemaphoreType.DMA((devices,)),
            pltpu.SemaphoreType.DMA((devices,)),
            pltpu.SemaphoreType.DMA((devices,)),
            pltpu.SemaphoreType.DMA((devices,)),
            pltpu.SemaphoreType.DMA((devices,)),
            pltpu.SemaphoreType.DMA((devices,)),
        ],
        compiler_params=pltpu.CompilerParams(
            collective_id=0, has_side_effects=True, vmem_limit_bytes=40 * 1024 * 1024
        ),
    )(lengths, asked, keys, values)


def on_device(
    queries,
    request_image,
    image_slot,
    image_lengths,
    image_keys,
    image_values,
    text_keys,
    text_values,
    text_lengths,
):
    rows, local_heads, head_size = queries.shape
    local_kv = image_keys.shape[1]
    group = local_heads // local_kv
    images = image_slot.shape[0]
    held = image_keys.shape[0]
    text_tokens = text_keys.shape[2]
    devices = lax.axis_size("seq")
    most = max(2, 2 * rows // images)
    slots_each = held * most
    scale = 1.0 / math.sqrt(head_size)
    me = lax.axis_index("seq")
    image_ids = jnp.arange(images, dtype=jnp.int32)
    chosen = request_image == image_ids[None, :]
    slots = jnp.sum(jnp.where(chosen, image_slot[None, :], 0), axis=1)
    slots = (slots + (devices - me) * held) % images
    slot_hits = (slots[:, None] == image_ids[None, :]).astype(jnp.int32)
    ranks = jnp.sum(slot_hits * (jnp.cumsum(slot_hits, axis=0) - 1), axis=1)
    targets = slots * most + ranks
    dispatch = (jnp.arange(images * most, dtype=jnp.int32)[:, None] == targets[None, :]).astype(
        jnp.bfloat16
    )
    by_head = queries.transpose(1, 0, 2)
    asked = jnp.einsum("sr,hrd->hsd", dispatch, by_head, preferred_element_type=jnp.float32)
    asked = asked.astype(jnp.bfloat16).reshape(local_heads, devices, slots_each, head_size)
    asked = asked.transpose(1, 0, 2, 3).reshape(devices, local_kv, group * slots_each, head_size)
    back, back_lse = exchange(asked, image_keys, image_values, image_lengths, devices, most, scale)
    back = back.reshape(devices, local_heads, slots_each, head_size).transpose(1, 0, 2, 3)
    back = back.reshape(local_heads, images * most, head_size)
    image_part = jnp.einsum("sr,hsd->rhd", dispatch, back, preferred_element_type=jnp.float32)
    image_part = image_part.reshape(rows, local_kv, group, head_size)
    back_lse = back_lse.reshape(devices * slots_each, 16)[:, :local_heads]
    image_lse = jnp.einsum(
        "sr,sc->rc", dispatch.astype(jnp.float32), back_lse, precision=lax.Precision.HIGHEST
    )
    image_lse = image_lse.reshape(rows, local_kv, group)
    heads = queries.reshape(rows, local_kv, group, head_size)
    scores = (
        jnp.einsum("rhgd,rhtd->rhgt", heads, text_keys, preferred_element_type=jnp.float32) * scale
    )
    valid = (jnp.arange(text_tokens, dtype=jnp.int32)[None, :] < text_lengths[:, None])[
        :, None, None, :
    ]
    weights, total, highest = weigh(scores, valid)
    text_out = (
        jnp.einsum("rhgt,rhtd->rhgd", weights, text_values, preferred_element_type=jnp.float32)
        / total
    )
    text_lse = highest[..., 0] + jnp.log(total[..., 0])
    upper = jnp.maximum(image_lse, text_lse)
    image_weight = jnp.exp(image_lse - upper)[..., None]
    text_weight = jnp.exp(text_lse - upper)[..., None]
    merged = (image_weight * image_part + text_weight * text_out) / (image_weight + text_weight)
    return merged.reshape(rows, local_heads, head_size).astype(jnp.bfloat16)


def solution(mesh):
    in_specs = (
        P(("groups", "seq"), "head", None),
        P(("groups", "seq"), None),
        P("groups"),
        P(("groups", "seq")),
        P(("groups", "seq"), "head", None, None),
        P(("groups", "seq"), "head", None, None),
        P(("groups", "seq"), "head", None, None),
        P(("groups", "seq"), "head", None, None),
        P(("groups", "seq")),
    )
    out_specs = P(("groups", "seq"), "head", None)
    return jax.shard_map(
        on_device, mesh=mesh, in_specs=in_specs, out_specs=out_specs, check_vma=False
    )
```

```python
import functools
import math

import jax
import jax.numpy as jnp
from jax import lax
from jax.experimental import pallas as pl
from jax.experimental.pallas import tpu as pltpu
from jax.sharding import PartitionSpec as P

NEGATIVE = -1e30
MESH = pl.DeviceIdType.MESH
CHUNK = 16


def iota(shape, axis):
    return lax.broadcasted_iota(jnp.int32, shape, axis).astype(jnp.float32)


def column(line):
    size = line.shape[1]
    same = iota((size, size), 0) == iota((size, size), 1)
    return jnp.sum(jnp.where(same, line, 0.0), axis=1, keepdims=True)


def kernel(
    devices,
    most,
    scale,
    lengths_ref,
    named_ref,
    slot_ref,
    text_lengths_ref,
    queries_hbm,
    image_keys_hbm,
    image_values_hbm,
    text_keys_hbm,
    text_values_hbm,
    out_ref,
    queries,
    keys,
    values,
    text_keys,
    text_values,
    bias,
    pick,
    asked,
    incoming,
    answer,
    answer_lse,
    back,
    back_lse,
    text_out,
    text_lse,
    query_sem,
    load_sem,
    text_sem,
    ask_send,
    ask_recv,
    out_send,
    out_recv,
    lse_send,
    lse_recv,
):
    held, local_kv, tokens, size = image_keys_hbm.shape
    heads, rows, _ = queries_hbm.shape
    text_tokens = text_keys_hbm.shape[2]
    images = slot_ref.shape[1]
    slots = held * most
    group = heads // local_kv
    me = lax.axis_index("seq")
    others = devices - 1

    def place(step):
        half = devices // 2 - (step + 1) // 2
        return half + (step % 2 == 0) * (devices - 2 * half)

    def ask(at):
        return pltpu.make_async_remote_copy(
            src_ref=asked.at[at],
            dst_ref=incoming.at[at],
            send_sem=ask_send.at[at],
            recv_sem=ask_recv.at[at],
            device_id={"seq": (me + at) % devices},
            device_id_type=MESH,
        )

    def reply(at):
        target = {"seq": (me + devices - at) % devices}
        return (
            pltpu.make_async_remote_copy(
                src_ref=answer.at[at],
                dst_ref=back.at[at],
                send_sem=out_send.at[at],
                recv_sem=out_recv.at[at],
                device_id=target,
                device_id_type=MESH,
            ),
            pltpu.make_async_remote_copy(
                src_ref=answer_lse.at[at],
                dst_ref=back_lse.at[at],
                send_sem=lse_send.at[at],
                recv_sem=lse_recv.at[at],
                device_id=target,
                device_id_type=MESH,
            ),
        )

    barrier = pltpu.get_barrier_semaphore()

    def greet(step, carry):
        pl.semaphore_signal(
            barrier, inc=1, device_id={"seq": (me + 1 + step) % devices}, device_id_type=MESH
        )
        return carry

    lax.fori_loop(0, others, greet, 0)

    first = pltpu.make_async_copy(queries_hbm, queries, query_sem)
    first.start()
    loads = []
    for image in range(held):
        for head in range(local_kv):
            for number, (source, target) in enumerate(
                ((image_keys_hbm, keys), (image_values_hbm, values))
            ):
                loads.append(
                    pltpu.make_async_copy(
                        source.at[image, head],
                        target.at[head, pl.ds(image * tokens, tokens)],
                        load_sem.at[number, image, head],
                    )
                )
    loads.append(pltpu.make_async_copy(text_keys_hbm, text_keys, text_sem.at[0]))
    loads.append(pltpu.make_async_copy(text_values_hbm, text_values, text_sem.at[1]))
    for load in loads:
        load.start()

    named = named_ref[...].astype(jnp.float32)
    slot_column = column(slot_ref[...].astype(jnp.float32))
    slot_of = jnp.where(iota((images, rows), 0) == named, slot_column, 0.0)
    slot_of = jnp.sum(slot_of, axis=0, keepdims=True)
    near = slot_of + ((devices - me) * held).astype(jnp.float32)
    near = jnp.where(near >= images, near - images, near)
    near_column = column(near)
    same = near_column == near
    earlier = iota((rows, rows), 0) < iota((rows, rows), 1)
    rank = jnp.sum(jnp.where(same & earlier, 1.0, 0.0), axis=0, keepdims=True)
    target_row = near * most + rank
    target = column(target_row)
    place_in = jnp.where(iota((images * most, rows), 0) == target_row, 1.0, 0.0)
    place_in = place_in.astype(jnp.bfloat16)
    pick[...] = jnp.where(iota((rows, images * most), 1) == target, 1.0, 0.0).astype(jnp.bfloat16)
    first.wait()
    for head in range(heads):
        sent = jnp.dot(place_in, queries[head], preferred_element_type=jnp.float32)
        sent = sent.reshape(devices, slots, size).astype(jnp.bfloat16)
        asked[:, head // group, pl.ds(head % group * slots, slots), :] = sent

    row = lax.broadcasted_iota(jnp.int32, (slots, held * tokens), 0)
    token = lax.broadcasted_iota(jnp.int32, (slots, held * tokens), 1)
    valid = jnp.zeros((slots, held * tokens), jnp.bool_)
    for image in range(held):
        mine = (row >= image * most) & (row < (image + 1) * most)
        inside = (token >= image * tokens) & (token < image * tokens + lengths_ref[image])
        valid = valid | (mine & inside)
    bias[...] = jnp.where(valid, 0.0, NEGATIVE)

    pl.semaphore_wait(barrier, others)

    def start_ask(step, carry):
        ask(place(step)).start()
        return carry

    lax.fori_loop(0, others, start_ask, 0)
    for load in loads:
        load.wait()

    text_length = column(text_lengths_ref[...].astype(jnp.float32))
    text_lse[...] = jnp.broadcast_to(text_length, text_lse.shape)
    wide = CHUNK * text_tokens
    lane = lax.broadcasted_iota(jnp.int32, (CHUNK, 128), 1)

    def read_text(chunk, carry):
        start = pl.multiple_of(chunk * CHUNK, CHUNK)
        limit = text_lse[pl.ds(start, CHUNK), :][:, :1]
        ahead = iota((CHUNK, wide), 1) - iota((CHUNK, wide), 0) * text_tokens
        text_bias = jnp.where((ahead >= 0) & (ahead < limit), 0.0, NEGATIVE)
        packed = jnp.zeros((CHUNK, 128), jnp.float32)
        for kv in range(local_kv):
            asking = queries[kv * group : (kv + 1) * group, pl.ds(start, CHUNK), :]
            asking = asking.reshape(group * CHUNK, size)
            those = text_keys[pl.ds(start, CHUNK), kv].reshape(wide, size)
            scores = lax.dot_general(
                asking, those, (((1,), (1,)), ((), ())), preferred_element_type=jnp.float32
            )
            scores = scores.reshape(group, CHUNK, wide) * scale + text_bias[None]
            highest = jnp.max(scores, axis=-1, keepdims=True)
            weights = jnp.exp(scores - highest)
            total = jnp.sum(weights, axis=-1, keepdims=True)
            weights = weights.astype(jnp.bfloat16).reshape(group * CHUNK, wide)
            those = text_values[pl.ds(start, CHUNK), kv].reshape(wide, size)
            mixed = jnp.dot(weights, those, preferred_element_type=jnp.float32)
            mixed = mixed.reshape(group, CHUNK, size) / total
            text_out[kv * group : (kv + 1) * group, pl.ds(start, CHUNK), :] = mixed
            lse = highest + jnp.log(total)
            for member in range(group):
                packed = jnp.where(lane == kv * group + member, lse[member], packed)
        text_lse[pl.ds(start, CHUNK), :] = packed
        return carry

    lax.fori_loop(0, rows // CHUNK, read_text, 0)

    spot = lax.broadcasted_iota(jnp.int32, (slots, 128), 1) - 16 * lax.broadcasted_iota(
        jnp.int32, (slots, 128), 0
    )

    def attend(read, at, out_to, lse_to):
        packed = jnp.zeros((slots, 128), jnp.float32)
        for head in range(local_kv):
            scores = lax.dot_general(
                read[at, head],
                keys[head],
                (((1,), (1,)), ((), ())),
                preferred_element_type=jnp.float32,
            )
            scores = scores.reshape(group, slots, held * tokens) * scale + bias[...][None]
            highest = jnp.max(scores, axis=-1, keepdims=True)
            weights = jnp.exp(scores - highest)
            total = jnp.sum(weights, axis=-1, keepdims=True)
            weights = weights.astype(jnp.bfloat16).reshape(group * slots, held * tokens)
            mixed = jnp.dot(weights, values[head], preferred_element_type=jnp.float32)
            mixed = mixed / total.reshape(group * slots, 1)
            out_to[at, head] = mixed.astype(jnp.bfloat16)
            lse = highest + jnp.log(total)
            for member in range(group):
                packed = jnp.where(spot == head * group + member, lse[member], packed)
        lse_to[at] = jnp.sum(packed, axis=0, keepdims=True)

    attend(asked, 0, back, back_lse)

    def serve(step, carry):
        @pl.when(step > 0)
        def _():
            for copy in reply(place(step - 1)):
                copy.start()

        at = place(step)
        ask(at).wait_recv()
        attend(incoming, at, answer, answer_lse)
        return carry

    lax.fori_loop(0, others, serve, 0)
    for copy in reply(place(others - 1)):
        copy.start()

    def finish(step, carry):
        at = place(step)
        ask(at).wait_send()
        for copy in reply(at):
            copy.wait()
        return carry

    lax.fori_loop(0, others, finish, 0)

    target = column(target_row)
    from_at = iota((rows, devices), 1) * slots
    from_here = jnp.where((target >= from_at) & (target < from_at + slots), 1.0, 0.0)
    chosen = jnp.dot(
        from_here,
        back_lse[...].reshape(devices, 128),
        precision=lax.Precision.HIGHEST,
        preferred_element_type=jnp.float32,
    )
    offset = jnp.sum(from_here * from_at, axis=1, keepdims=True)
    start = (target - offset) * 16
    lanes = iota((rows, 128), 1)
    chosen = jnp.where((lanes >= start) & (lanes < start + 16), chosen, 0.0)
    fold = iota((128, 128), 0) - iota((128, 128), 1)
    landed = jnp.zeros((128, 128), jnp.float32)
    for line in range(slots):
        landed = jnp.where(fold == 16 * line, 1.0, landed)
    landed = jnp.where(iota((128, 128), 1) < 16, landed, 0.0)
    image_lse = jnp.dot(
        chosen, landed, precision=lax.Precision.HIGHEST, preferred_element_type=jnp.float32
    )
    top = jnp.maximum(image_lse, text_lse[...])
    image_weight = jnp.exp(image_lse - top)
    text_weight = jnp.exp(text_lse[...] - top)
    whole = image_weight + text_weight
    for head in range(heads):
        came = back[:, head // group, pl.ds(head % group * slots, slots), :]
        came = came.astype(jnp.float32).reshape(devices * slots, size).astype(jnp.bfloat16)
        image_out = jnp.dot(pick[...], came, preferred_element_type=jnp.float32)
        merged = image_weight[:, head : head + 1] * image_out
        merged = merged + text_weight[:, head : head + 1] * text_out[head]
        out_ref[head] = (merged / whole[:, head : head + 1]).astype(jnp.bfloat16)


def on_device(
    queries,
    request_image,
    image_slot,
    image_lengths,
    image_keys,
    image_values,
    text_keys,
    text_values,
    text_lengths,
):
    rows, heads, size = queries.shape
    held, local_kv, tokens, _ = image_keys.shape
    images = image_slot.shape[0]
    devices = lax.axis_size("seq")
    most = max(2, 2 * rows // images)
    slots = held * most
    scale = 1.0 / math.sqrt(size)
    message = (devices, local_kv, heads // local_kv * slots, size)
    vmem = pl.BlockSpec(memory_space=pltpu.VMEM)
    hbm = pl.BlockSpec(memory_space=pl.ANY)
    links = pltpu.SemaphoreType.DMA((devices,))
    out = pl.pallas_call(
        functools.partial(kernel, devices, most, scale),
        out_shape=jax.ShapeDtypeStruct((heads, rows, size), jnp.bfloat16),
        in_specs=[pl.BlockSpec(memory_space=pltpu.SMEM), vmem, vmem, vmem, hbm, hbm, hbm, hbm, hbm],
        out_specs=vmem,
        scratch_shapes=[
            pltpu.VMEM((heads, rows, size), jnp.bfloat16),
            pltpu.VMEM((local_kv, held * tokens, size), jnp.bfloat16),
            pltpu.VMEM((local_kv, held * tokens, size), jnp.bfloat16),
            pltpu.VMEM(text_keys.shape, jnp.bfloat16),
            pltpu.VMEM(text_values.shape, jnp.bfloat16),
            pltpu.VMEM((slots, held * tokens), jnp.float32),
            pltpu.VMEM((rows, images * most), jnp.bfloat16),
            pltpu.VMEM(message, jnp.bfloat16),
            pltpu.VMEM(message, jnp.bfloat16),
            pltpu.VMEM(message, jnp.bfloat16),
            pltpu.VMEM((devices, 1, 128), jnp.float32),
            pltpu.VMEM(message, jnp.bfloat16),
            pltpu.VMEM((devices, 1, 128), jnp.float32),
            pltpu.VMEM((heads, rows, size), jnp.float32),
            pltpu.VMEM((rows, 128), jnp.float32),
            pltpu.SemaphoreType.DMA,
            pltpu.SemaphoreType.DMA((2, held, local_kv)),
            pltpu.SemaphoreType.DMA((2,)),
            links,
            links,
            links,
            links,
            links,
            links,
        ],
        compiler_params=pltpu.CompilerParams(
            collective_id=0, has_side_effects=True, vmem_limit_bytes=62 * 1024 * 1024
        ),
    )(
        image_lengths,
        request_image.reshape(1, rows),
        image_slot.reshape(1, images),
        text_lengths.reshape(1, rows),
        queries.transpose(1, 0, 2),
        image_keys,
        image_values,
        text_keys,
        text_values,
    )
    return out.transpose(1, 0, 2)


def solution(mesh):
    in_specs = (
        P(("groups", "seq"), "head", None),
        P(("groups", "seq"), None),
        P("groups"),
        P(("groups", "seq")),
        P(("groups", "seq"), "head", None, None),
        P(("groups", "seq"), "head", None, None),
        P(("groups", "seq"), "head", None, None),
        P(("groups", "seq"), "head", None, None),
        P(("groups", "seq")),
    )
    out_specs = P(("groups", "seq"), "head", None)
    return jax.shard_map(
        on_device, mesh=mesh, in_specs=in_specs, out_specs=out_specs, check_vma=False
    )
```

```python
import functools
import math

import jax
import jax.numpy as jnp
from jax import lax
from jax.experimental import pallas as pl
from jax.experimental.pallas import tpu as pltpu
from jax.sharding import PartitionSpec as P

NEGATIVE = -1e30
MESH = pl.DeviceIdType.MESH
CHUNK = 16


def iota(shape, axis):
    return lax.broadcasted_iota(jnp.int32, shape, axis).astype(jnp.float32)


def column(line):
    size = line.shape[1]
    same = iota((size, size), 0) == iota((size, size), 1)
    return jnp.sum(jnp.where(same, line, 0.0), axis=1, keepdims=True)


def kernel(
    devices,
    most,
    scale,
    lengths_ref,
    named_ref,
    slot_ref,
    text_lengths_ref,
    queries_hbm,
    image_keys_hbm,
    image_values_hbm,
    text_keys_hbm,
    text_values_hbm,
    out_ref,
    queries,
    keys,
    values,
    text_keys,
    text_values,
    bias,
    pick,
    asked,
    incoming,
    answer,
    answer_lse,
    back,
    back_lse,
    text_out,
    text_lse,
    far_sem,
    query_sem,
    load_sem,
    text_sem,
    ask_send,
    ask_recv,
    out_send,
    out_recv,
    lse_send,
    lse_recv,
):
    held, local_kv, tokens, size = image_keys_hbm.shape
    heads, rows, _ = queries_hbm.shape
    text_tokens = text_keys_hbm.shape[2]
    images = slot_ref.shape[1]
    slots = held * most
    group = heads // local_kv
    me = lax.axis_index("seq")
    others = devices - 1

    reach = devices // 4
    close = 2 * reach

    def near_place(step):
        hops = reach - step // 2
        return hops + (step % 2) * (devices - 2 * hops)

    def far_place(step):
        hops = devices // 2 - (step + 1) // 2
        return hops + (1 - step % 2) * (devices - 2 * hops)

    def ask(at):
        return pltpu.make_async_remote_copy(
            src_ref=asked.at[at],
            dst_ref=incoming.at[at],
            send_sem=ask_send.at[at],
            recv_sem=ask_recv.at[at],
            device_id={"seq": (me + at) % devices},
            device_id_type=MESH,
        )

    def reply(at):
        target = {"seq": (me + devices - at) % devices}
        return (
            pltpu.make_async_remote_copy(
                src_ref=answer.at[at],
                dst_ref=back.at[at],
                send_sem=out_send.at[at],
                recv_sem=out_recv.at[at],
                device_id=target,
                device_id_type=MESH,
            ),
            pltpu.make_async_remote_copy(
                src_ref=answer_lse.at[at],
                dst_ref=back_lse.at[at],
                send_sem=lse_send.at[at],
                recv_sem=lse_recv.at[at],
                device_id=target,
                device_id_type=MESH,
            ),
        )

    barrier = pltpu.get_barrier_semaphore()

    def greet(step, carry):
        pl.semaphore_signal(
            barrier,
            inc=1,
            device_id={"seq": (me + near_place(step)) % devices},
            device_id_type=MESH,
        )
        return carry

    lax.fori_loop(0, close, greet, 0)

    first = pltpu.make_async_copy(queries_hbm, queries, query_sem)
    first.start()
    loads = []
    for image in range(held):
        for head in range(local_kv):
            for number, (source, target) in enumerate(
                ((image_keys_hbm, keys), (image_values_hbm, values))
            ):
                loads.append(
                    pltpu.make_async_copy(
                        source.at[image, head],
                        target.at[head, pl.ds(image * tokens, tokens)],
                        load_sem.at[number, image, head],
                    )
                )
    loads.append(pltpu.make_async_copy(text_keys_hbm, text_keys, text_sem.at[0]))
    loads.append(pltpu.make_async_copy(text_values_hbm, text_values, text_sem.at[1]))
    for load in loads:
        load.start()

    named = named_ref[...].astype(jnp.float32)
    slot_column = column(slot_ref[...].astype(jnp.float32))
    slot_of = jnp.where(iota((images, rows), 0) == named, slot_column, 0.0)
    slot_of = jnp.sum(slot_of, axis=0, keepdims=True)
    near = slot_of + ((devices - me) * held).astype(jnp.float32)
    near = jnp.where(near >= images, near - images, near)
    near_column = column(near)
    same = near_column == near
    earlier = iota((rows, rows), 0) < iota((rows, rows), 1)
    rank = jnp.sum(jnp.where(same & earlier, 1.0, 0.0), axis=0, keepdims=True)
    target_row = near * most + rank
    target = column(target_row)
    place_in = jnp.where(iota((images * most, rows), 0) == target_row, 1.0, 0.0)
    place_in = place_in.astype(jnp.bfloat16)
    pick[...] = jnp.where(iota((rows, images * most), 1) == target, 1.0, 0.0).astype(jnp.bfloat16)
    first.wait()
    for head in range(heads):
        sent = jnp.dot(place_in, queries[head], preferred_element_type=jnp.float32)
        sent = sent.reshape(devices, slots, size).astype(jnp.bfloat16)
        asked[:, head // group, pl.ds(head % group * slots, slots), :] = sent

    row = lax.broadcasted_iota(jnp.int32, (slots, held * tokens), 0)
    token = lax.broadcasted_iota(jnp.int32, (slots, held * tokens), 1)
    valid = jnp.zeros((slots, held * tokens), jnp.bool_)
    for image in range(held):
        mine = (row >= image * most) & (row < (image + 1) * most)
        inside = (token >= image * tokens) & (token < image * tokens + lengths_ref[image])
        valid = valid | (mine & inside)
    bias[...] = jnp.where(valid, 0.0, NEGATIVE)

    pl.semaphore_wait(barrier, close)
    for step in range(2):
        pl.semaphore_signal(
            far_sem,
            inc=1,
            device_id={"seq": (me + near_place(step)) % devices},
            device_id_type=MESH,
        )

    def ask_near(step, carry):
        ask(near_place(step)).start()
        return carry

    lax.fori_loop(0, close, ask_near, 0)
    for load in loads:
        load.wait()

    text_length = column(text_lengths_ref[...].astype(jnp.float32))
    text_lse[...] = jnp.broadcast_to(text_length, text_lse.shape)
    wide = CHUNK * text_tokens
    lane = lax.broadcasted_iota(jnp.int32, (CHUNK, 128), 1)

    def read_text(chunk, carry):
        start = pl.multiple_of(chunk * CHUNK, CHUNK)
        limit = text_lse[pl.ds(start, CHUNK), :][:, :1]
        ahead = iota((CHUNK, wide), 1) - iota((CHUNK, wide), 0) * text_tokens
        text_bias = jnp.where((ahead >= 0) & (ahead < limit), 0.0, NEGATIVE)
        packed = jnp.zeros((CHUNK, 128), jnp.float32)
        for kv in range(local_kv):
            asking = queries[kv * group : (kv + 1) * group, pl.ds(start, CHUNK), :]
            asking = asking.reshape(group * CHUNK, size)
            those = text_keys[pl.ds(start, CHUNK), kv].reshape(wide, size)
            scores = lax.dot_general(
                asking, those, (((1,), (1,)), ((), ())), preferred_element_type=jnp.float32
            )
            scores = scores.reshape(group, CHUNK, wide) * scale + text_bias[None]
            highest = jnp.max(scores, axis=-1, keepdims=True)
            weights = jnp.exp(scores - highest)
            total = jnp.sum(weights, axis=-1, keepdims=True)
            weights = weights.astype(jnp.bfloat16).reshape(group * CHUNK, wide)
            those = text_values[pl.ds(start, CHUNK), kv].reshape(wide, size)
            mixed = jnp.dot(weights, those, preferred_element_type=jnp.float32)
            mixed = mixed.reshape(group, CHUNK, size) / total
            text_out[kv * group : (kv + 1) * group, pl.ds(start, CHUNK), :] = mixed
            lse = highest + jnp.log(total)
            for member in range(group):
                packed = jnp.where(lane == kv * group + member, lse[member], packed)
        text_lse[pl.ds(start, CHUNK), :] = packed
        return carry

    lax.fori_loop(0, rows // CHUNK, read_text, 0)
    pl.semaphore_wait(far_sem, 2)

    def ask_far(step, carry):
        ask(far_place(step)).start()
        return carry

    lax.fori_loop(0, others - close, ask_far, 0)

    spot = lax.broadcasted_iota(jnp.int32, (slots, 128), 1) - 16 * lax.broadcasted_iota(
        jnp.int32, (slots, 128), 0
    )

    def attend(read, at, out_to, lse_to):
        packed = jnp.zeros((slots, 128), jnp.float32)
        for head in range(local_kv):
            scores = lax.dot_general(
                read[at, head],
                keys[head],
                (((1,), (1,)), ((), ())),
                preferred_element_type=jnp.float32,
            )
            scores = scores.reshape(group, slots, held * tokens) * scale + bias[...][None]
            highest = jnp.max(scores, axis=-1, keepdims=True)
            weights = jnp.exp(scores - highest)
            total = jnp.sum(weights, axis=-1, keepdims=True)
            weights = weights.astype(jnp.bfloat16).reshape(group * slots, held * tokens)
            mixed = jnp.dot(weights, values[head], preferred_element_type=jnp.float32)
            mixed = mixed / total.reshape(group * slots, 1)
            out_to[at, head] = mixed.astype(jnp.bfloat16)
            lse = highest + jnp.log(total)
            for member in range(group):
                packed = jnp.where(spot == head * group + member, lse[member], packed)
        lse_to[at] = jnp.sum(packed, axis=0, keepdims=True)

    attend(asked, 0, back, back_lse)

    def serve(at):
        ask(at).wait_recv()
        attend(incoming, at, answer, answer_lse)

    def send_back(at):
        for copy in reply(at):
            copy.start()

    def serve_near(step, carry):
        serve(near_place(step))
        return carry

    def serve_far(step, carry):
        @pl.when(step > 0)
        def _():
            send_back(far_place(step - 1))

        serve(far_place(step))
        return carry

    def send_near(step, carry):
        send_back(near_place(step))
        return carry

    lax.fori_loop(0, close, serve_near, 0)
    lax.fori_loop(0, others - close, serve_far, 0)
    send_back(far_place(others - close - 1))
    lax.fori_loop(0, close, send_near, 0)

    def finish(step, carry):
        ask(step).wait_send()
        for copy in reply(step):
            copy.wait()
        return carry

    lax.fori_loop(1, devices, finish, 0)

    target = column(target_row)
    from_at = iota((rows, devices), 1) * slots
    from_here = jnp.where((target >= from_at) & (target < from_at + slots), 1.0, 0.0)
    chosen = jnp.dot(
        from_here,
        back_lse[...].reshape(devices, 128),
        precision=lax.Precision.HIGHEST,
        preferred_element_type=jnp.float32,
    )
    offset = jnp.sum(from_here * from_at, axis=1, keepdims=True)
    start = (target - offset) * 16
    lanes = iota((rows, 128), 1)
    chosen = jnp.where((lanes >= start) & (lanes < start + 16), chosen, 0.0)
    fold = iota((128, 128), 0) - iota((128, 128), 1)
    landed = jnp.zeros((128, 128), jnp.float32)
    for line in range(slots):
        landed = jnp.where(fold == 16 * line, 1.0, landed)
    landed = jnp.where(iota((128, 128), 1) < 16, landed, 0.0)
    image_lse = jnp.dot(
        chosen, landed, precision=lax.Precision.HIGHEST, preferred_element_type=jnp.float32
    )
    top = jnp.maximum(image_lse, text_lse[...])
    image_weight = jnp.exp(image_lse - top)
    text_weight = jnp.exp(text_lse[...] - top)
    whole = image_weight + text_weight
    for head in range(heads):
        came = back[:, head // group, pl.ds(head % group * slots, slots), :]
        came = came.astype(jnp.float32).reshape(devices * slots, size).astype(jnp.bfloat16)
        image_out = jnp.dot(pick[...], came, preferred_element_type=jnp.float32)
        merged = image_weight[:, head : head + 1] * image_out
        merged = merged + text_weight[:, head : head + 1] * text_out[head]
        out_ref[head] = (merged / whole[:, head : head + 1]).astype(jnp.bfloat16)


def on_device(
    queries,
    request_image,
    image_slot,
    image_lengths,
    image_keys,
    image_values,
    text_keys,
    text_values,
    text_lengths,
):
    rows, heads, size = queries.shape
    held, local_kv, tokens, _ = image_keys.shape
    images = image_slot.shape[0]
    devices = lax.axis_size("seq")
    most = max(2, 2 * rows // images)
    slots = held * most
    scale = 1.0 / math.sqrt(size)
    message = (devices, local_kv, heads // local_kv * slots, size)
    vmem = pl.BlockSpec(memory_space=pltpu.VMEM)
    hbm = pl.BlockSpec(memory_space=pl.ANY)
    links = pltpu.SemaphoreType.DMA((devices,))
    out = pl.pallas_call(
        functools.partial(kernel, devices, most, scale),
        out_shape=jax.ShapeDtypeStruct((heads, rows, size), jnp.bfloat16),
        in_specs=[pl.BlockSpec(memory_space=pltpu.SMEM), vmem, vmem, vmem, hbm, hbm, hbm, hbm, hbm],
        out_specs=vmem,
        scratch_shapes=[
            pltpu.VMEM((heads, rows, size), jnp.bfloat16),
            pltpu.VMEM((local_kv, held * tokens, size), jnp.bfloat16),
            pltpu.VMEM((local_kv, held * tokens, size), jnp.bfloat16),
            pltpu.VMEM(text_keys.shape, jnp.bfloat16),
            pltpu.VMEM(text_values.shape, jnp.bfloat16),
            pltpu.VMEM((slots, held * tokens), jnp.float32),
            pltpu.VMEM((rows, images * most), jnp.bfloat16),
            pltpu.VMEM(message, jnp.bfloat16),
            pltpu.VMEM(message, jnp.bfloat16),
            pltpu.VMEM(message, jnp.bfloat16),
            pltpu.VMEM((devices, 1, 128), jnp.float32),
            pltpu.VMEM(message, jnp.bfloat16),
            pltpu.VMEM((devices, 1, 128), jnp.float32),
            pltpu.VMEM((heads, rows, size), jnp.float32),
            pltpu.VMEM((rows, 128), jnp.float32),
            pltpu.SemaphoreType.REGULAR,
            pltpu.SemaphoreType.DMA,
            pltpu.SemaphoreType.DMA((2, held, local_kv)),
            pltpu.SemaphoreType.DMA((2,)),
            links,
            links,
            links,
            links,
            links,
            links,
        ],
        compiler_params=pltpu.CompilerParams(
            collective_id=0, has_side_effects=True, vmem_limit_bytes=62 * 1024 * 1024
        ),
    )(
        image_lengths,
        request_image.reshape(1, rows),
        image_slot.reshape(1, images),
        text_lengths.reshape(1, rows),
        queries.transpose(1, 0, 2),
        image_keys,
        image_values,
        text_keys,
        text_values,
    )
    return out.transpose(1, 0, 2)


def solution(mesh):
    in_specs = (
        P(("groups", "seq"), "head", None),
        P(("groups", "seq"), None),
        P("groups"),
        P(("groups", "seq")),
        P(("groups", "seq"), "head", None, None),
        P(("groups", "seq"), "head", None, None),
        P(("groups", "seq"), "head", None, None),
        P(("groups", "seq"), "head", None, None),
        P(("groups", "seq")),
    )
    out_specs = P(("groups", "seq"), "head", None)
    return jax.shard_map(
        on_device, mesh=mesh, in_specs=in_specs, out_specs=out_specs, check_vma=False
    )
```

```python
import functools
import math

import jax
import jax.numpy as jnp
from jax import lax
from jax.experimental import pallas as pl
from jax.experimental.pallas import tpu as pltpu
from jax.sharding import PartitionSpec as P

NEGATIVE = -1e30
MESH = pl.DeviceIdType.MESH
CHUNK = 16


def iota(shape, axis):
    return lax.broadcasted_iota(jnp.int32, shape, axis).astype(jnp.float32)


def column(line):
    size = line.shape[1]
    same = iota((size, size), 0) == iota((size, size), 1)
    return jnp.sum(jnp.where(same, line, 0.0), axis=1, keepdims=True)


def kernel(
    devices,
    most,
    scale,
    lengths_hbm,
    named_hbm,
    slot_hbm,
    text_lengths_hbm,
    queries_hbm,
    image_keys_hbm,
    image_values_hbm,
    text_keys_hbm,
    text_values_hbm,
    out_ref,
    lengths_ref,
    named_ref,
    slot_ref,
    text_lengths_ref,
    queries,
    keys,
    values,
    text_keys,
    text_values,
    bias,
    pick,
    asked,
    incoming,
    answer,
    answer_lse,
    back,
    back_lse,
    text_out,
    text_lse,
    far_sem,
    first_sem,
    load_sem,
    text_sem,
    ask_send,
    ask_recv,
    out_send,
    out_recv,
    lse_send,
    lse_recv,
):
    held, local_kv, tokens, size = image_keys_hbm.shape
    heads, rows, _ = queries_hbm.shape
    text_tokens = text_keys_hbm.shape[2]
    images = slot_hbm.shape[1]
    slots = held * most
    group = heads // local_kv
    me = lax.axis_index("seq")
    others = devices - 1

    reach = devices // 4
    close = 2 * reach
    stages = [(0, 2)]
    while stages[-1][1] < reach:
        stages.append((stages[-1][1], 2 * stages[-1][1]))

    def both(hops, step):
        return hops + (step % 2) * (devices - 2 * hops)

    def near_place(step):
        turn = step // 2
        hops, before = -turn, 0
        for low, high in stages:
            hops = hops + (turn >= low) * (low + high - before)
            before = low + high
        return both(hops, step)

    def far_place(step):
        hops = devices // 2 - (step + 1) // 2
        return hops + (1 - step % 2) * (devices - 2 * hops)

    def ask(at):
        return pltpu.make_async_remote_copy(
            src_ref=asked.at[at],
            dst_ref=incoming.at[at],
            send_sem=ask_send.at[at],
            recv_sem=ask_recv.at[at],
            device_id={"seq": (me + at) % devices},
            device_id_type=MESH,
        )

    def reply(at):
        target = {"seq": (me + devices - at) % devices}
        return (
            pltpu.make_async_remote_copy(
                src_ref=answer.at[at],
                dst_ref=back.at[at],
                send_sem=out_send.at[at],
                recv_sem=out_recv.at[at],
                device_id=target,
                device_id_type=MESH,
            ),
            pltpu.make_async_remote_copy(
                src_ref=answer_lse.at[at],
                dst_ref=back_lse.at[at],
                send_sem=lse_send.at[at],
                recv_sem=lse_recv.at[at],
                device_id=target,
                device_id_type=MESH,
            ),
        )

    def signal(sem, hops):
        for at in (hops, devices - hops):
            pl.semaphore_signal(
                sem, inc=1, device_id={"seq": (me + at) % devices}, device_id_type=MESH
            )

    first = [
        pltpu.make_async_copy(source, target, first_sem.at[number])
        for number, (source, target) in enumerate(
            (
                (named_hbm, named_ref),
                (slot_hbm, slot_ref),
                (queries_hbm, queries),
                (lengths_hbm, lengths_ref),
                (text_lengths_hbm, text_lengths_ref),
            )
        )
    ]
    for load in first:
        load.start()
    barrier = pltpu.get_barrier_semaphore()
    signal(barrier, 1)
    signal(barrier, 2)

    loads = []
    for image in range(held):
        for head in range(local_kv):
            for number, (source, target) in enumerate(
                ((image_keys_hbm, keys), (image_values_hbm, values))
            ):
                loads.append(
                    pltpu.make_async_copy(
                        source.at[image, head],
                        target.at[head, pl.ds(image * tokens, tokens)],
                        load_sem.at[number, image, head],
                    )
                )
    loads.append(pltpu.make_async_copy(text_keys_hbm, text_keys, text_sem.at[0]))
    loads.append(pltpu.make_async_copy(text_values_hbm, text_values, text_sem.at[1]))
    first[0].wait()
    first[1].wait()
    named = named_ref[...].astype(jnp.float32)
    slot_column = column(slot_ref[...].astype(jnp.float32))
    slot_of = jnp.where(iota((images, rows), 0) == named, slot_column, 0.0)
    slot_of = jnp.sum(slot_of, axis=0, keepdims=True)
    near = slot_of + ((devices - me) * held).astype(jnp.float32)
    near = jnp.where(near >= images, near - images, near)
    near_column = column(near)
    same = near_column == near
    earlier = iota((rows, rows), 0) < iota((rows, rows), 1)
    rank = jnp.sum(jnp.where(same & earlier, 1.0, 0.0), axis=0, keepdims=True)
    target_row = near * most + rank
    target = column(target_row)
    place_in = jnp.where(iota((images * most, rows), 0) == target_row, 1.0, 0.0)
    place_in = place_in.astype(jnp.bfloat16)
    pick[...] = jnp.where(iota((rows, images * most), 1) == target, 1.0, 0.0).astype(jnp.bfloat16)
    first[2].wait()
    for load in loads:
        load.start()
    for head in range(heads):
        sent = jnp.dot(place_in, queries[head], preferred_element_type=jnp.float32)
        sent = sent.reshape(devices, slots, size).astype(jnp.bfloat16)
        asked[:, head // group, pl.ds(head % group * slots, slots), :] = sent

    def ask_near(step, carry):
        ask(near_place(step)).start()
        return carry

    for stage, (low, high) in enumerate(stages):
        if stage == 0:
            pl.semaphore_wait(barrier, 4)
        else:
            pl.semaphore_wait(far_sem.at[stage - 1], 2)
        signal(far_sem.at[stage], high)
        lax.fori_loop(2 * low, 2 * high, ask_near, 0)

    first[3].wait()
    first[4].wait()
    row = lax.broadcasted_iota(jnp.int32, (slots, held * tokens), 0)
    token = lax.broadcasted_iota(jnp.int32, (slots, held * tokens), 1)
    valid = jnp.zeros((slots, held * tokens), jnp.bool_)
    for image in range(held):
        mine = (row >= image * most) & (row < (image + 1) * most)
        inside = (token >= image * tokens) & (token < image * tokens + lengths_ref[image])
        valid = valid | (mine & inside)
    bias[...] = jnp.where(valid, 0.0, NEGATIVE)

    for load in loads:
        load.wait()

    text_length = column(text_lengths_ref[...].astype(jnp.float32))
    text_lse[...] = jnp.broadcast_to(text_length, text_lse.shape)
    wide = CHUNK * text_tokens
    lane = lax.broadcasted_iota(jnp.int32, (CHUNK, 128), 1)

    def read_text(chunk, carry):
        start = pl.multiple_of(chunk * CHUNK, CHUNK)
        limit = text_lse[pl.ds(start, CHUNK), :][:, :1]
        ahead = iota((CHUNK, wide), 1) - iota((CHUNK, wide), 0) * text_tokens
        text_bias = jnp.where((ahead >= 0) & (ahead < limit), 0.0, NEGATIVE)
        packed = jnp.zeros((CHUNK, 128), jnp.float32)
        for kv in range(local_kv):
            asking = queries[kv * group : (kv + 1) * group, pl.ds(start, CHUNK), :]
            asking = asking.reshape(group * CHUNK, size)
            those = text_keys[pl.ds(start, CHUNK), kv].reshape(wide, size)
            scores = lax.dot_general(
                asking, those, (((1,), (1,)), ((), ())), preferred_element_type=jnp.float32
            )
            scores = scores.reshape(group, CHUNK, wide) * scale + text_bias[None]
            highest = jnp.max(scores, axis=-1, keepdims=True)
            weights = jnp.exp(scores - highest)
            total = jnp.sum(weights, axis=-1, keepdims=True)
            weights = weights.astype(jnp.bfloat16).reshape(group * CHUNK, wide)
            those = text_values[pl.ds(start, CHUNK), kv].reshape(wide, size)
            mixed = jnp.dot(weights, those, preferred_element_type=jnp.float32)
            mixed = mixed.reshape(group, CHUNK, size) / total
            text_out[kv * group : (kv + 1) * group, pl.ds(start, CHUNK), :] = mixed
            lse = highest + jnp.log(total)
            for member in range(group):
                packed = jnp.where(lane == kv * group + member, lse[member], packed)
        text_lse[pl.ds(start, CHUNK), :] = packed
        return carry

    lax.fori_loop(0, rows // CHUNK, read_text, 0)
    pl.semaphore_wait(far_sem.at[len(stages) - 1], 2)

    def ask_far(step, carry):
        ask(far_place(step)).start()
        return carry

    lax.fori_loop(0, others - close, ask_far, 0)

    spot = lax.broadcasted_iota(jnp.int32, (slots, 128), 1) - 16 * lax.broadcasted_iota(
        jnp.int32, (slots, 128), 0
    )

    def attend(read, at, out_to, lse_to):
        packed = jnp.zeros((slots, 128), jnp.float32)
        for head in range(local_kv):
            scores = lax.dot_general(
                read[at, head],
                keys[head],
                (((1,), (1,)), ((), ())),
                preferred_element_type=jnp.float32,
            )
            scores = scores.reshape(group, slots, held * tokens) * scale + bias[...][None]
            highest = jnp.max(scores, axis=-1, keepdims=True)
            weights = jnp.exp(scores - highest)
            total = jnp.sum(weights, axis=-1, keepdims=True)
            weights = weights.astype(jnp.bfloat16).reshape(group * slots, held * tokens)
            mixed = jnp.dot(weights, values[head], preferred_element_type=jnp.float32)
            mixed = mixed / total.reshape(group * slots, 1)
            out_to[at, head] = mixed.astype(jnp.bfloat16)
            lse = highest + jnp.log(total)
            for member in range(group):
                packed = jnp.where(spot == head * group + member, lse[member], packed)
        lse_to[at] = jnp.sum(packed, axis=0, keepdims=True)

    attend(asked, 0, back, back_lse)

    def serve(at):
        ask(at).wait_recv()
        attend(incoming, at, answer, answer_lse)

    def send_back(at):
        for copy in reply(at):
            copy.start()

    def serve_near(step, carry):
        serve(near_place(step))
        return carry

    def serve_far(step, carry):
        @pl.when(step > 0)
        def _():
            send_back(far_place(step - 1))

        serve(far_place(step))
        return carry

    def send_near(step, carry):
        send_back(both(reach - step // 2, step))
        return carry

    def left(step, carry):
        ask(step).wait_send()
        return carry

    lax.fori_loop(0, close, serve_near, 0)
    lax.fori_loop(0, others - close, serve_far, 0)
    send_back(far_place(others - close - 1))
    lax.fori_loop(0, close, send_near, 0)
    lax.fori_loop(1, devices, left, 0)

    def finish(step, carry):
        for copy in reply(step):
            copy.wait()
        return carry

    lax.fori_loop(1, devices, finish, 0)

    target = column(target_row)
    from_at = iota((rows, devices), 1) * slots
    from_here = jnp.where((target >= from_at) & (target < from_at + slots), 1.0, 0.0)
    chosen = jnp.dot(
        from_here,
        back_lse[...].reshape(devices, 128),
        precision=lax.Precision.HIGHEST,
        preferred_element_type=jnp.float32,
    )
    offset = jnp.sum(from_here * from_at, axis=1, keepdims=True)
    start = (target - offset) * 16
    lanes = iota((rows, 128), 1)
    chosen = jnp.where((lanes >= start) & (lanes < start + 16), chosen, 0.0)
    fold = iota((128, 128), 0) - iota((128, 128), 1)
    landed = jnp.zeros((128, 128), jnp.float32)
    for line in range(slots):
        landed = jnp.where(fold == 16 * line, 1.0, landed)
    landed = jnp.where(iota((128, 128), 1) < 16, landed, 0.0)
    image_lse = jnp.dot(
        chosen, landed, precision=lax.Precision.HIGHEST, preferred_element_type=jnp.float32
    )
    top = jnp.maximum(image_lse, text_lse[...])
    image_weight = jnp.exp(image_lse - top)
    text_weight = jnp.exp(text_lse[...] - top)
    whole = image_weight + text_weight
    for head in range(heads):
        came = back[:, head // group, pl.ds(head % group * slots, slots), :]
        came = came.astype(jnp.float32).reshape(devices * slots, size).astype(jnp.bfloat16)
        image_out = jnp.dot(pick[...], came, preferred_element_type=jnp.float32)
        merged = image_weight[:, head : head + 1] * image_out
        merged = merged + text_weight[:, head : head + 1] * text_out[head]
        out_ref[head] = (merged / whole[:, head : head + 1]).astype(jnp.bfloat16)


def on_device(
    queries,
    request_image,
    image_slot,
    image_lengths,
    image_keys,
    image_values,
    text_keys,
    text_values,
    text_lengths,
):
    rows, heads, size = queries.shape
    held, local_kv, tokens, _ = image_keys.shape
    images = image_slot.shape[0]
    devices = lax.axis_size("seq")
    most = max(2, 2 * rows // images)
    slots = held * most
    scale = 1.0 / math.sqrt(size)
    message = (devices, local_kv, heads // local_kv * slots, size)
    vmem = pl.BlockSpec(memory_space=pltpu.VMEM)
    hbm = pl.BlockSpec(memory_space=pltpu.HBM)
    links = pltpu.SemaphoreType.DMA((devices,))
    out = pl.pallas_call(
        functools.partial(kernel, devices, most, scale),
        out_shape=jax.ShapeDtypeStruct((heads, rows, size), jnp.bfloat16),
        in_specs=[hbm] * 9,
        out_specs=vmem,
        scratch_shapes=[
            pltpu.SMEM((held,), jnp.int32),
            pltpu.VMEM((1, rows), jnp.int32),
            pltpu.VMEM((1, images), jnp.int32),
            pltpu.VMEM((1, rows), jnp.int32),
            pltpu.VMEM((heads, rows, size), jnp.bfloat16),
            pltpu.VMEM((local_kv, held * tokens, size), jnp.bfloat16),
            pltpu.VMEM((local_kv, held * tokens, size), jnp.bfloat16),
            pltpu.VMEM(text_keys.shape, jnp.bfloat16),
            pltpu.VMEM(text_values.shape, jnp.bfloat16),
            pltpu.VMEM((slots, held * tokens), jnp.float32),
            pltpu.VMEM((rows, images * most), jnp.bfloat16),
            pltpu.VMEM(message, jnp.bfloat16),
            pltpu.VMEM(message, jnp.bfloat16),
            pltpu.VMEM(message, jnp.bfloat16),
            pltpu.VMEM((devices, 1, 128), jnp.float32),
            pltpu.VMEM(message, jnp.bfloat16),
            pltpu.VMEM((devices, 1, 128), jnp.float32),
            pltpu.VMEM((heads, rows, size), jnp.float32),
            pltpu.VMEM((rows, 128), jnp.float32),
            pltpu.SemaphoreType.REGULAR((8,)),
            pltpu.SemaphoreType.DMA((5,)),
            pltpu.SemaphoreType.DMA((2, held, local_kv)),
            pltpu.SemaphoreType.DMA((2,)),
            links,
            links,
            links,
            links,
            links,
            links,
        ],
        compiler_params=pltpu.CompilerParams(
            collective_id=0, has_side_effects=True, vmem_limit_bytes=32 * 1024 * 1024
        ),
    )(
        *(
            pltpu.with_memory_space_constraint(array, pltpu.HBM)
            for array in (
                image_lengths,
                request_image.reshape(1, rows),
                image_slot.reshape(1, images),
                text_lengths.reshape(1, rows),
                queries.transpose(1, 0, 2),
                image_keys,
                image_values,
                text_keys,
                text_values,
            )
        )
    )
    return out.transpose(1, 0, 2)


def solution(mesh):
    in_specs = (
        P(("groups", "seq"), "head", None),
        P(("groups", "seq"), None),
        P("groups"),
        P(("groups", "seq")),
        P(("groups", "seq"), "head", None, None),
        P(("groups", "seq"), "head", None, None),
        P(("groups", "seq"), "head", None, None),
        P(("groups", "seq"), "head", None, None),
        P(("groups", "seq")),
    )
    out_specs = P(("groups", "seq"), "head", None)
    return jax.shard_map(
        on_device, mesh=mesh, in_specs=in_specs, out_specs=out_specs, check_vma=False
    )
```

```python
import functools
import math

import jax
import jax.numpy as jnp
from jax import lax
from jax.experimental import pallas as pl
from jax.experimental.pallas import tpu as pltpu
from jax.sharding import PartitionSpec as P

NEGATIVE = -1e30
MESH = pl.DeviceIdType.MESH
CHUNK = 16


def iota(shape, axis):
    return lax.broadcasted_iota(jnp.int32, shape, axis).astype(jnp.float32)


def column(line):
    size = line.shape[1]
    same = iota((size, size), 0) == iota((size, size), 1)
    return jnp.sum(jnp.where(same, line, 0.0), axis=1, keepdims=True)


def kernel(
    devices,
    most,
    scale,
    lengths_hbm,
    named_hbm,
    slot_hbm,
    text_lengths_hbm,
    queries_hbm,
    image_keys_hbm,
    image_values_hbm,
    text_keys_hbm,
    text_values_hbm,
    out_ref,
    lengths_ref,
    named_ref,
    slot_ref,
    text_lengths_ref,
    queries,
    keys,
    values,
    text_keys,
    text_values,
    bias,
    pick,
    asked,
    incoming,
    answer,
    answer_lse,
    back,
    back_lse,
    text_out,
    shares,
    text_lse,
    far_sem,
    first_sem,
    load_sem,
    text_sem,
    ask_send,
    ask_recv,
    out_send,
    out_recv,
    lse_send,
    lse_recv,
):
    held, local_kv, tokens, size = image_keys_hbm.shape
    heads, rows, _ = queries_hbm.shape
    text_tokens = text_keys_hbm.shape[2]
    images = slot_hbm.shape[1]
    slots = held * most
    group = heads // local_kv
    me = lax.axis_index("seq")
    others = devices - 1

    reach = devices // 4
    close = 2 * reach
    stages = [(0, 2)]
    while stages[-1][1] < reach:
        stages.append((stages[-1][1], 2 * stages[-1][1]))

    def both(hops, step):
        return hops + (step % 2) * (devices - 2 * hops)

    def near_place(step):
        turn = step // 2
        hops, before = -turn, 0
        for low, high in stages:
            hops = hops + (turn >= low) * (low + high - before)
            before = low + high
        return both(hops, step)

    def far_place(step):
        hops = devices // 2 - (step + 1) // 2
        return hops + (1 - step % 2) * (devices - 2 * hops)

    def ask(at):
        return pltpu.make_async_remote_copy(
            src_ref=asked.at[at],
            dst_ref=incoming.at[at],
            send_sem=ask_send.at[at],
            recv_sem=ask_recv.at[at],
            device_id={"seq": (me + at) % devices},
            device_id_type=MESH,
        )

    def reply(at):
        return pltpu.make_async_remote_copy(
            src_ref=answer.at[at],
            dst_ref=back.at[at],
            send_sem=out_send.at[at],
            recv_sem=out_recv.at[at],
            device_id={"seq": (me + devices - at) % devices},
            device_id_type=MESH,
        )

    def reply_lse(at):
        return pltpu.make_async_remote_copy(
            src_ref=answer_lse.at[at],
            dst_ref=back_lse.at[at],
            send_sem=lse_send.at[at],
            recv_sem=lse_recv.at[at],
            device_id={"seq": (me + devices - at) % devices},
            device_id_type=MESH,
        )

    def signal(sem, hops):
        for at in (hops, devices - hops):
            pl.semaphore_signal(
                sem, inc=1, device_id={"seq": (me + at) % devices}, device_id_type=MESH
            )

    first = [
        pltpu.make_async_copy(source, target, first_sem.at[number])
        for number, (source, target) in enumerate(
            (
                (named_hbm, named_ref),
                (slot_hbm, slot_ref),
                (queries_hbm, queries),
                (lengths_hbm, lengths_ref),
                (text_lengths_hbm, text_lengths_ref),
            )
        )
    ]
    for load in first:
        load.start()
    barrier = pltpu.get_barrier_semaphore()
    signal(barrier, 1)
    signal(barrier, 2)

    loads = []
    for image in range(held):
        for head in range(local_kv):
            for number, (source, target) in enumerate(
                ((image_keys_hbm, keys), (image_values_hbm, values))
            ):
                loads.append(
                    pltpu.make_async_copy(
                        source.at[image, head],
                        target.at[head, pl.ds(image * tokens, tokens)],
                        load_sem.at[number, image, head],
                    )
                )
    loads.append(pltpu.make_async_copy(text_keys_hbm, text_keys, text_sem.at[0]))
    loads.append(pltpu.make_async_copy(text_values_hbm, text_values, text_sem.at[1]))
    first[0].wait()
    first[1].wait()
    named = named_ref[...].astype(jnp.float32)
    slot_column = column(slot_ref[...].astype(jnp.float32))
    slot_of = jnp.where(iota((images, rows), 0) == named, slot_column, 0.0)
    slot_of = jnp.sum(slot_of, axis=0, keepdims=True)
    near = slot_of + ((devices - me) * held).astype(jnp.float32)
    near = jnp.where(near >= images, near - images, near)
    near_column = column(near)
    same = near_column == near
    earlier = iota((rows, rows), 0) < iota((rows, rows), 1)
    rank = jnp.sum(jnp.where(same & earlier, 1.0, 0.0), axis=0, keepdims=True)
    target_row = near * most + rank
    target = column(target_row)
    place_in = jnp.where(iota((images * most, rows), 0) == target_row, 1.0, 0.0)
    place_in = place_in.astype(jnp.bfloat16)
    pick[...] = jnp.where(iota((rows, images * most), 1) == target, 1.0, 0.0).astype(jnp.bfloat16)
    first[2].wait()
    for load in loads:
        load.start()
    for head in range(heads):
        sent = jnp.dot(place_in, queries[head], preferred_element_type=jnp.float32)
        sent = sent.reshape(devices, slots, size).astype(jnp.bfloat16)
        asked[:, head // group, pl.ds(head % group * slots, slots), :] = sent

    def ask_near(step, carry):
        ask(near_place(step)).start()
        return carry

    for stage, (low, high) in enumerate(stages):
        if stage == 0:
            pl.semaphore_wait(barrier, 4)
        else:
            pl.semaphore_wait(far_sem.at[stage - 1], 2)
        signal(far_sem.at[stage], high)
        lax.fori_loop(2 * low, 2 * high, ask_near, 0)

    first[3].wait()
    first[4].wait()
    row = lax.broadcasted_iota(jnp.int32, (slots, held * tokens), 0)
    token = lax.broadcasted_iota(jnp.int32, (slots, held * tokens), 1)
    valid = jnp.zeros((slots, held * tokens), jnp.bool_)
    for image in range(held):
        mine = (row >= image * most) & (row < (image + 1) * most)
        inside = (token >= image * tokens) & (token < image * tokens + lengths_ref[image])
        valid = valid | (mine & inside)
    bias[...] = jnp.where(valid, 0.0, NEGATIVE)

    for load in loads:
        load.wait()

    text_length = column(text_lengths_ref[...].astype(jnp.float32))
    text_lse[...] = jnp.broadcast_to(text_length, text_lse.shape)
    wide = CHUNK * text_tokens
    lane = lax.broadcasted_iota(jnp.int32, (CHUNK, 128), 1)

    def read_text(chunk, carry):
        start = pl.multiple_of(chunk * CHUNK, CHUNK)
        limit = text_lse[pl.ds(start, CHUNK), :][:, :1]
        ahead = iota((CHUNK, wide), 1) - iota((CHUNK, wide), 0) * text_tokens
        text_bias = jnp.where((ahead >= 0) & (ahead < limit), 0.0, NEGATIVE)
        packed = jnp.zeros((CHUNK, 128), jnp.float32)
        for kv in range(local_kv):
            asking = queries[kv * group : (kv + 1) * group, pl.ds(start, CHUNK), :]
            asking = asking.reshape(group * CHUNK, size)
            those = text_keys[pl.ds(start, CHUNK), kv].reshape(wide, size)
            scores = lax.dot_general(
                asking, those, (((1,), (1,)), ((), ())), preferred_element_type=jnp.float32
            )
            scores = scores.reshape(group, CHUNK, wide) * scale + text_bias[None]
            highest = jnp.max(scores, axis=-1, keepdims=True)
            weights = jnp.exp(scores - highest)
            total = jnp.sum(weights, axis=-1, keepdims=True)
            weights = weights.astype(jnp.bfloat16).reshape(group * CHUNK, wide)
            those = text_values[pl.ds(start, CHUNK), kv].reshape(wide, size)
            mixed = jnp.dot(weights, those, preferred_element_type=jnp.float32)
            mixed = mixed.reshape(group, CHUNK, size) / total
            text_out[kv * group : (kv + 1) * group, pl.ds(start, CHUNK), :] = mixed
            lse = highest + jnp.log(total)
            for member in range(group):
                packed = jnp.where(lane == kv * group + member, lse[member], packed)
        text_lse[pl.ds(start, CHUNK), :] = packed
        return carry

    lax.fori_loop(0, rows // CHUNK, read_text, 0)
    pl.semaphore_wait(far_sem.at[len(stages) - 1], 2)

    def ask_far(step, carry):
        ask(far_place(step)).start()
        return carry

    lax.fori_loop(0, others - close, ask_far, 0)

    spot = lax.broadcasted_iota(jnp.int32, (slots, 128), 1) - 16 * lax.broadcasted_iota(
        jnp.int32, (slots, 128), 0
    )

    def attend(read, at, out_to, lse_to):
        packed = jnp.zeros((slots, 128), jnp.float32)
        for head in range(local_kv):
            scores = lax.dot_general(
                read[at, head],
                keys[head],
                (((1,), (1,)), ((), ())),
                preferred_element_type=jnp.float32,
            )
            scores = scores.reshape(group, slots, held * tokens) * scale + bias[...][None]
            highest = jnp.max(scores, axis=-1, keepdims=True)
            weights = jnp.exp(scores - highest)
            total = jnp.sum(weights, axis=-1, keepdims=True)
            weights = weights.astype(jnp.bfloat16).reshape(group * slots, held * tokens)
            mixed = jnp.dot(weights, values[head], preferred_element_type=jnp.float32)
            mixed = mixed / total.reshape(group * slots, 1)
            out_to[at, head] = mixed.astype(jnp.bfloat16)
            lse = highest + jnp.log(total)
            for member in range(group):
                packed = jnp.where(spot == head * group + member, lse[member], packed)
        lse_to[at] = jnp.sum(packed, axis=0, keepdims=True)

    attend(asked, 0, back, back_lse)

    def serve(at):
        ask(at).wait_recv()
        attend(incoming, at, answer, answer_lse)

    def serve_near(step, carry):
        @pl.when(step > 0)
        def _():
            reply_lse(near_place(step - 1)).start()

        serve(near_place(step))
        return carry

    def serve_far(step, carry):
        @pl.when(step > 0)
        def _():
            reply(far_place(step - 1)).start()
            reply_lse(far_place(step - 1)).start()

        serve(far_place(step))
        return carry

    def send_near(step, carry):
        reply(both(reach - step // 2, step)).start()
        return carry

    lax.fori_loop(0, close, serve_near, 0)
    reply_lse(near_place(close - 1)).start()
    lax.fori_loop(0, others - close, serve_far, 0)
    reply(far_place(others - close - 1)).start()
    reply_lse(far_place(others - close - 1)).start()
    lax.fori_loop(0, close, send_near, 0)

    def settle(step, carry):
        ask(step).wait_send()
        reply_lse(step).wait()
        return carry

    def finish(step, carry):
        reply(step).wait()
        return carry

    lax.fori_loop(1, devices, settle, 0)

    target = column(target_row)
    from_at = iota((rows, devices), 1) * slots
    from_here = jnp.where((target >= from_at) & (target < from_at + slots), 1.0, 0.0)
    chosen = jnp.dot(
        from_here,
        back_lse[...].reshape(devices, 128),
        precision=lax.Precision.HIGHEST,
        preferred_element_type=jnp.float32,
    )
    offset = jnp.sum(from_here * from_at, axis=1, keepdims=True)
    start = (target - offset) * 16
    lanes = iota((rows, 128), 1)
    chosen = jnp.where((lanes >= start) & (lanes < start + 16), chosen, 0.0)
    fold = iota((128, 128), 0) - iota((128, 128), 1)
    landed = jnp.zeros((128, 128), jnp.float32)
    for line in range(slots):
        landed = jnp.where(fold == 16 * line, 1.0, landed)
    landed = jnp.where(iota((128, 128), 1) < 16, landed, 0.0)
    image_lse = jnp.dot(
        chosen, landed, precision=lax.Precision.HIGHEST, preferred_element_type=jnp.float32
    )
    top = jnp.maximum(image_lse, text_lse[...])
    image_weight = jnp.exp(image_lse - top)
    text_weight = jnp.exp(text_lse[...] - top)
    whole = image_weight + text_weight
    image_share = image_weight / whole
    text_share = text_weight / whole
    for head in range(heads):
        text_out[head] = text_out[head] * text_share[:, head : head + 1]
        shares[head] = jnp.broadcast_to(image_share[:, head : head + 1], (rows, size))

    lax.fori_loop(reach + 1, devices - reach, finish, 0)
    lax.fori_loop(1, reach + 1, finish, 0)
    lax.fori_loop(devices - reach, devices, finish, 0)
    for head in range(heads):
        came = back[:, head // group, pl.ds(head % group * slots, slots), :]
        came = came.reshape(devices * slots, size)
        image_out = jnp.dot(pick[...], came, preferred_element_type=jnp.float32)
        out_ref[head] = (shares[head] * image_out + text_out[head]).astype(jnp.bfloat16)


def on_device(
    queries,
    request_image,
    image_slot,
    image_lengths,
    image_keys,
    image_values,
    text_keys,
    text_values,
    text_lengths,
):
    rows, heads, size = queries.shape
    held, local_kv, tokens, _ = image_keys.shape
    images = image_slot.shape[0]
    devices = lax.axis_size("seq")
    most = max(2, 2 * rows // images)
    slots = held * most
    scale = 1.0 / math.sqrt(size)
    message = (devices, local_kv, heads // local_kv * slots, size)
    vmem = pl.BlockSpec(memory_space=pltpu.VMEM)
    hbm = pl.BlockSpec(memory_space=pltpu.HBM)
    links = pltpu.SemaphoreType.DMA((devices,))
    out = pl.pallas_call(
        functools.partial(kernel, devices, most, scale),
        out_shape=jax.ShapeDtypeStruct((heads, rows, size), jnp.bfloat16),
        in_specs=[hbm] * 9,
        out_specs=vmem,
        scratch_shapes=[
            pltpu.SMEM((held,), jnp.int32),
            pltpu.VMEM((1, rows), jnp.int32),
            pltpu.VMEM((1, images), jnp.int32),
            pltpu.VMEM((1, rows), jnp.int32),
            pltpu.VMEM((heads, rows, size), jnp.bfloat16),
            pltpu.VMEM((local_kv, held * tokens, size), jnp.bfloat16),
            pltpu.VMEM((local_kv, held * tokens, size), jnp.bfloat16),
            pltpu.VMEM(text_keys.shape, jnp.bfloat16),
            pltpu.VMEM(text_values.shape, jnp.bfloat16),
            pltpu.VMEM((slots, held * tokens), jnp.float32),
            pltpu.VMEM((rows, images * most), jnp.bfloat16),
            pltpu.VMEM(message, jnp.bfloat16),
            pltpu.VMEM(message, jnp.bfloat16),
            pltpu.VMEM(message, jnp.bfloat16),
            pltpu.VMEM((devices, 1, 128), jnp.float32),
            pltpu.VMEM(message, jnp.bfloat16),
            pltpu.VMEM((devices, 1, 128), jnp.float32),
            pltpu.VMEM((heads, rows, size), jnp.float32),
            pltpu.VMEM((heads, rows, size), jnp.float32),
            pltpu.VMEM((rows, 128), jnp.float32),
            pltpu.SemaphoreType.REGULAR((8,)),
            pltpu.SemaphoreType.DMA((5,)),
            pltpu.SemaphoreType.DMA((2, held, local_kv)),
            pltpu.SemaphoreType.DMA((2,)),
            links,
            links,
            links,
            links,
            links,
            links,
        ],
        compiler_params=pltpu.CompilerParams(
            collective_id=0, has_side_effects=True, vmem_limit_bytes=32 * 1024 * 1024
        ),
    )(
        *(
            pltpu.with_memory_space_constraint(array, pltpu.HBM)
            for array in (
                image_lengths,
                request_image.reshape(1, rows),
                image_slot.reshape(1, images),
                text_lengths.reshape(1, rows),
                queries.transpose(1, 0, 2),
                image_keys,
                image_values,
                text_keys,
                text_values,
            )
        )
    )
    return out.transpose(1, 0, 2)


def solution(mesh):
    in_specs = (
        P(("groups", "seq"), "head", None),
        P(("groups", "seq"), None),
        P("groups"),
        P(("groups", "seq")),
        P(("groups", "seq"), "head", None, None),
        P(("groups", "seq"), "head", None, None),
        P(("groups", "seq"), "head", None, None),
        P(("groups", "seq"), "head", None, None),
        P(("groups", "seq")),
    )
    out_specs = P(("groups", "seq"), "head", None)
    return jax.shard_map(
        on_device, mesh=mesh, in_specs=in_specs, out_specs=out_specs, check_vma=False
    )
```

```python
import functools
import math

import jax
import jax.numpy as jnp
from jax import lax
from jax.experimental import pallas as pl
from jax.experimental.pallas import tpu as pltpu
from jax.sharding import PartitionSpec as P

NEGATIVE = -1e30
MESH = pl.DeviceIdType.MESH
CHUNK = 16


def iota(shape, axis):
    return lax.broadcasted_iota(jnp.int32, shape, axis).astype(jnp.float32)


def column(line):
    size = line.shape[1]
    same = iota((size, size), 0) == iota((size, size), 1)
    return jnp.sum(jnp.where(same, line, 0.0), axis=1, keepdims=True)


def kernel(
    devices,
    most,
    scale,
    lengths_hbm,
    named_hbm,
    slot_hbm,
    text_lengths_hbm,
    queries_hbm,
    image_keys_hbm,
    image_values_hbm,
    text_keys_hbm,
    text_values_hbm,
    out_ref,
    lengths_ref,
    named_ref,
    slot_ref,
    text_lengths_ref,
    queries,
    keys,
    values,
    text_keys,
    text_values,
    bias,
    pick,
    asked,
    incoming,
    answer,
    answer_lse,
    back,
    back_lse,
    text_out,
    shares,
    text_lse,
    far_sem,
    first_sem,
    load_sem,
    text_sem,
    ask_send,
    ask_recv,
    out_send,
    out_recv,
    lse_send,
    lse_recv,
):
    held, local_kv, tokens, size = image_keys_hbm.shape
    heads, rows, _ = queries_hbm.shape
    text_tokens = text_keys_hbm.shape[2]
    images = slot_hbm.shape[1]
    slots = held * most
    group = heads // local_kv
    me = lax.axis_index("seq")
    others = devices - 1

    reach = devices // 4
    close = 2 * reach
    stages = [(0, 2)]
    while stages[-1][1] < reach:
        stages.append((stages[-1][1], 2 * stages[-1][1]))

    def both(hops, step):
        return hops + (step % 2) * (devices - 2 * hops)

    def near_place(step):
        turn = step // 2
        hops, before = -turn, 0
        for low, high in stages:
            hops = hops + (turn >= low) * (low + high - before)
            before = low + high
        return both(hops, step)

    def far_place(step):
        hops = devices // 2 - (step + 1) // 2
        return hops + (1 - step % 2) * (devices - 2 * hops)

    def ask(at):
        return pltpu.make_async_remote_copy(
            src_ref=asked.at[at],
            dst_ref=incoming.at[at],
            send_sem=ask_send.at[at],
            recv_sem=ask_recv.at[at],
            device_id={"seq": (me + at) % devices},
            device_id_type=MESH,
        )

    def reply(at):
        return pltpu.make_async_remote_copy(
            src_ref=answer.at[at],
            dst_ref=back.at[at],
            send_sem=out_send.at[at],
            recv_sem=out_recv.at[at],
            device_id={"seq": (me + devices - at) % devices},
            device_id_type=MESH,
        )

    def reply_lse(at):
        return pltpu.make_async_remote_copy(
            src_ref=answer_lse.at[at],
            dst_ref=back_lse.at[at],
            send_sem=lse_send.at[at],
            recv_sem=lse_recv.at[at],
            device_id={"seq": (me + devices - at) % devices},
            device_id_type=MESH,
        )

    def signal(sem, hops):
        for at in (hops, devices - hops):
            pl.semaphore_signal(
                sem, inc=1, device_id={"seq": (me + at) % devices}, device_id_type=MESH
            )

    first = [
        pltpu.make_async_copy(source, target, first_sem.at[number])
        for number, (source, target) in enumerate(
            (
                (named_hbm, named_ref),
                (slot_hbm, slot_ref),
                (queries_hbm, queries),
                (lengths_hbm, lengths_ref),
                (text_lengths_hbm, text_lengths_ref),
            )
        )
    ]
    for load in first:
        load.start()
    barrier = pltpu.get_barrier_semaphore()
    signal(barrier, 1)
    signal(barrier, 2)

    loads = []
    for image in range(held):
        for head in range(local_kv):
            for number, (source, target) in enumerate(
                ((image_keys_hbm, keys), (image_values_hbm, values))
            ):
                loads.append(
                    pltpu.make_async_copy(
                        source.at[image, head],
                        target.at[head, pl.ds(image * tokens, tokens)],
                        load_sem.at[number, image, head],
                    )
                )
    loads.append(pltpu.make_async_copy(text_keys_hbm, text_keys, text_sem.at[0]))
    loads.append(pltpu.make_async_copy(text_values_hbm, text_values, text_sem.at[1]))
    first[0].wait()
    first[1].wait()
    named = named_ref[...].astype(jnp.float32)
    slot_column = column(slot_ref[...].astype(jnp.float32))
    slot_of = jnp.where(iota((images, rows), 0) == named, slot_column, 0.0)
    slot_of = jnp.sum(slot_of, axis=0, keepdims=True)
    near = slot_of + ((devices - me) * held).astype(jnp.float32)
    near = jnp.where(near >= images, near - images, near)
    near_column = column(near)
    same = near_column == near
    earlier = iota((rows, rows), 0) < iota((rows, rows), 1)
    rank = jnp.sum(jnp.where(same & earlier, 1.0, 0.0), axis=0, keepdims=True)
    target_row = near * most + rank
    pl.semaphore_wait(barrier, 4)
    signal(far_sem.at[0], stages[0][1])
    first[2].wait()
    for load in loads:
        load.start()

    def dispatch(ranges):
        for low, high in ranges:
            number = (high - low) * slots
            place_in = iota((number, rows), 0) + low * slots == target_row
            place_in = jnp.where(place_in, 1.0, 0.0).astype(jnp.bfloat16)
            for head in range(heads):
                sent = jnp.dot(place_in, queries[head], preferred_element_type=jnp.float32)
                sent = sent.reshape(high - low, slots, size).astype(jnp.bfloat16)
                asked[low:high, head // group, pl.ds(head % group * slots, slots), :] = sent

    dispatch(((0, reach + 1), (devices - reach, devices)))

    def ask_near(step, carry):
        ask(near_place(step)).start()
        return carry

    for stage, (low, high) in enumerate(stages):
        if stage > 0:
            pl.semaphore_wait(far_sem.at[stage - 1], 2)
            signal(far_sem.at[stage], high)
        lax.fori_loop(2 * low, 2 * high, ask_near, 0)

    dispatch(((reach + 1, devices - reach),))
    target = column(target_row)
    pick[...] = jnp.where(iota((rows, images * most), 1) == target, 1.0, 0.0).astype(jnp.bfloat16)
    first[3].wait()
    first[4].wait()
    row = lax.broadcasted_iota(jnp.int32, (slots, held * tokens), 0)
    token = lax.broadcasted_iota(jnp.int32, (slots, held * tokens), 1)
    valid = jnp.zeros((slots, held * tokens), jnp.bool_)
    for image in range(held):
        mine = (row >= image * most) & (row < (image + 1) * most)
        inside = (token >= image * tokens) & (token < image * tokens + lengths_ref[image])
        valid = valid | (mine & inside)
    bias[...] = jnp.where(valid, 0.0, NEGATIVE)

    for load in loads:
        load.wait()

    text_length = column(text_lengths_ref[...].astype(jnp.float32))
    text_lse[...] = jnp.broadcast_to(text_length, text_lse.shape)
    wide = CHUNK * text_tokens
    lane = lax.broadcasted_iota(jnp.int32, (CHUNK, 128), 1)

    def read_text(chunk, carry):
        start = pl.multiple_of(chunk * CHUNK, CHUNK)
        limit = text_lse[pl.ds(start, CHUNK), :][:, :1]
        ahead = iota((CHUNK, wide), 1) - iota((CHUNK, wide), 0) * text_tokens
        text_bias = jnp.where((ahead >= 0) & (ahead < limit), 0.0, NEGATIVE)
        packed = jnp.zeros((CHUNK, 128), jnp.float32)
        for kv in range(local_kv):
            asking = queries[kv * group : (kv + 1) * group, pl.ds(start, CHUNK), :]
            asking = asking.reshape(group * CHUNK, size)
            those = text_keys[pl.ds(start, CHUNK), kv].reshape(wide, size)
            scores = lax.dot_general(
                asking, those, (((1,), (1,)), ((), ())), preferred_element_type=jnp.float32
            )
            scores = scores.reshape(group, CHUNK, wide) * scale + text_bias[None]
            highest = jnp.max(scores, axis=-1, keepdims=True)
            weights = jnp.exp(scores - highest)
            total = jnp.sum(weights, axis=-1, keepdims=True)
            weights = weights.astype(jnp.bfloat16).reshape(group * CHUNK, wide)
            those = text_values[pl.ds(start, CHUNK), kv].reshape(wide, size)
            mixed = jnp.dot(weights, those, preferred_element_type=jnp.float32)
            mixed = mixed.reshape(group, CHUNK, size) / total
            text_out[kv * group : (kv + 1) * group, pl.ds(start, CHUNK), :] = mixed
            lse = highest + jnp.log(total)
            for member in range(group):
                packed = jnp.where(lane == kv * group + member, lse[member], packed)
        text_lse[pl.ds(start, CHUNK), :] = packed
        return carry

    lax.fori_loop(0, rows // CHUNK, read_text, 0)
    pl.semaphore_wait(far_sem.at[len(stages) - 1], 2)

    def ask_far(step, carry):
        ask(far_place(step)).start()
        return carry

    lax.fori_loop(0, others - close, ask_far, 0)

    spot = lax.broadcasted_iota(jnp.int32, (slots, 128), 1) - 16 * lax.broadcasted_iota(
        jnp.int32, (slots, 128), 0
    )

    def attend(read, at, out_to, lse_to):
        packed = jnp.zeros((slots, 128), jnp.float32)
        for head in range(local_kv):
            scores = lax.dot_general(
                read[at, head],
                keys[head],
                (((1,), (1,)), ((), ())),
                preferred_element_type=jnp.float32,
            )
            scores = scores.reshape(group, slots, held * tokens) * scale + bias[...][None]
            highest = jnp.max(scores, axis=-1, keepdims=True)
            weights = jnp.exp(scores - highest)
            total = jnp.sum(weights, axis=-1, keepdims=True)
            weights = weights.astype(jnp.bfloat16).reshape(group * slots, held * tokens)
            mixed = jnp.dot(weights, values[head], preferred_element_type=jnp.float32)
            mixed = mixed / total.reshape(group * slots, 1)
            out_to[at, head] = mixed.astype(jnp.bfloat16)
            lse = highest + jnp.log(total)
            for member in range(group):
                packed = jnp.where(spot == head * group + member, lse[member], packed)
        lse_to[at] = jnp.sum(packed, axis=0, keepdims=True)

    attend(asked, 0, back, back_lse)

    def serve(at):
        ask(at).wait_recv()
        attend(incoming, at, answer, answer_lse)

    def serve_near(step, carry):
        @pl.when(step > 0)
        def _():
            reply_lse(near_place(step - 1)).start()

        serve(near_place(step))
        return carry

    def serve_far(step, carry):
        @pl.when(step > 0)
        def _():
            reply(far_place(step - 1)).start()
            reply_lse(far_place(step - 1)).start()

        serve(far_place(step))
        return carry

    def send_near(step, carry):
        reply(both(reach - step // 2, step)).start()
        return carry

    lax.fori_loop(0, close, serve_near, 0)
    reply_lse(near_place(close - 1)).start()
    lax.fori_loop(0, others - close, serve_far, 0)
    reply(far_place(others - close - 1)).start()
    reply_lse(far_place(others - close - 1)).start()
    lax.fori_loop(0, close, send_near, 0)

    def settle(step, carry):
        ask(step).wait_send()
        reply_lse(step).wait()
        return carry

    def finish(step, carry):
        reply(step).wait()
        return carry

    lax.fori_loop(1, devices, settle, 0)

    target = column(target_row)
    from_at = iota((rows, devices), 1) * slots
    from_here = jnp.where((target >= from_at) & (target < from_at + slots), 1.0, 0.0)
    chosen = jnp.dot(
        from_here,
        back_lse[...].reshape(devices, 128),
        precision=lax.Precision.HIGHEST,
        preferred_element_type=jnp.float32,
    )
    offset = jnp.sum(from_here * from_at, axis=1, keepdims=True)
    start = (target - offset) * 16
    lanes = iota((rows, 128), 1)
    chosen = jnp.where((lanes >= start) & (lanes < start + 16), chosen, 0.0)
    fold = iota((128, 128), 0) - iota((128, 128), 1)
    landed = jnp.zeros((128, 128), jnp.float32)
    for line in range(slots):
        landed = jnp.where(fold == 16 * line, 1.0, landed)
    landed = jnp.where(iota((128, 128), 1) < 16, landed, 0.0)
    image_lse = jnp.dot(
        chosen, landed, precision=lax.Precision.HIGHEST, preferred_element_type=jnp.float32
    )
    top = jnp.maximum(image_lse, text_lse[...])
    image_weight = jnp.exp(image_lse - top)
    text_weight = jnp.exp(text_lse[...] - top)
    whole = image_weight + text_weight
    image_share = image_weight / whole
    text_share = text_weight / whole
    for head in range(heads):
        text_out[head] = text_out[head] * text_share[:, head : head + 1]
        shares[head] = jnp.broadcast_to(image_share[:, head : head + 1], (rows, size))

    lax.fori_loop(reach + 1, devices - reach, finish, 0)
    lax.fori_loop(1, reach + 1, finish, 0)
    lax.fori_loop(devices - reach, devices, finish, 0)
    for head in range(heads):
        came = back[:, head // group, pl.ds(head % group * slots, slots), :]
        came = came.reshape(devices * slots, size)
        image_out = jnp.dot(pick[...], came, preferred_element_type=jnp.float32)
        out_ref[head] = (shares[head] * image_out + text_out[head]).astype(jnp.bfloat16)


def on_device(
    queries,
    request_image,
    image_slot,
    image_lengths,
    image_keys,
    image_values,
    text_keys,
    text_values,
    text_lengths,
):
    rows, heads, size = queries.shape
    held, local_kv, tokens, _ = image_keys.shape
    images = image_slot.shape[0]
    devices = lax.axis_size("seq")
    most = max(2, 2 * rows // images)
    slots = held * most
    scale = 1.0 / math.sqrt(size)
    message = (devices, local_kv, heads // local_kv * slots, size)
    vmem = pl.BlockSpec(memory_space=pltpu.VMEM)
    hbm = pl.BlockSpec(memory_space=pltpu.HBM)
    links = pltpu.SemaphoreType.DMA((devices,))
    out = pl.pallas_call(
        functools.partial(kernel, devices, most, scale),
        out_shape=jax.ShapeDtypeStruct((heads, rows, size), jnp.bfloat16),
        in_specs=[hbm] * 9,
        out_specs=vmem,
        scratch_shapes=[
            pltpu.SMEM((held,), jnp.int32),
            pltpu.VMEM((1, rows), jnp.int32),
            pltpu.VMEM((1, images), jnp.int32),
            pltpu.VMEM((1, rows), jnp.int32),
            pltpu.VMEM((heads, rows, size), jnp.bfloat16),
            pltpu.VMEM((local_kv, held * tokens, size), jnp.bfloat16),
            pltpu.VMEM((local_kv, held * tokens, size), jnp.bfloat16),
            pltpu.VMEM(text_keys.shape, jnp.bfloat16),
            pltpu.VMEM(text_values.shape, jnp.bfloat16),
            pltpu.VMEM((slots, held * tokens), jnp.float32),
            pltpu.VMEM((rows, images * most), jnp.bfloat16),
            pltpu.VMEM(message, jnp.bfloat16),
            pltpu.VMEM(message, jnp.bfloat16),
            pltpu.VMEM(message, jnp.bfloat16),
            pltpu.VMEM((devices, 1, 128), jnp.float32),
            pltpu.VMEM(message, jnp.bfloat16),
            pltpu.VMEM((devices, 1, 128), jnp.float32),
            pltpu.VMEM((heads, rows, size), jnp.float32),
            pltpu.VMEM((heads, rows, size), jnp.float32),
            pltpu.VMEM((rows, 128), jnp.float32),
            pltpu.SemaphoreType.REGULAR((8,)),
            pltpu.SemaphoreType.DMA((5,)),
            pltpu.SemaphoreType.DMA((2, held, local_kv)),
            pltpu.SemaphoreType.DMA((2,)),
            links,
            links,
            links,
            links,
            links,
            links,
        ],
        compiler_params=pltpu.CompilerParams(
            collective_id=0, has_side_effects=True, vmem_limit_bytes=32 * 1024 * 1024
        ),
    )(
        *(
            pltpu.with_memory_space_constraint(array, pltpu.HBM)
            for array in (
                image_lengths,
                request_image.reshape(1, rows),
                image_slot.reshape(1, images),
                text_lengths.reshape(1, rows),
                queries.transpose(1, 0, 2),
                image_keys,
                image_values,
                text_keys,
                text_values,
            )
        )
    )
    return out.transpose(1, 0, 2)


def solution(mesh):
    in_specs = (
        P(("groups", "seq"), "head", None),
        P(("groups", "seq"), None),
        P("groups"),
        P(("groups", "seq")),
        P(("groups", "seq"), "head", None, None),
        P(("groups", "seq"), "head", None, None),
        P(("groups", "seq"), "head", None, None),
        P(("groups", "seq"), "head", None, None),
        P(("groups", "seq")),
    )
    out_specs = P(("groups", "seq"), "head", None)
    return jax.shard_map(
        on_device, mesh=mesh, in_specs=in_specs, out_specs=out_specs, check_vma=False
    )
```

```python
import functools
import math

import jax
import jax.numpy as jnp
from jax import lax
from jax.experimental import pallas as pl
from jax.experimental.pallas import tpu as pltpu
from jax.sharding import PartitionSpec as P

NEGATIVE = -1e30
MESH = pl.DeviceIdType.MESH
CHUNK = 16


def iota(shape, axis):
    return lax.broadcasted_iota(jnp.int32, shape, axis).astype(jnp.float32)


def column(line):
    size = line.shape[1]
    same = iota((size, size), 0) == iota((size, size), 1)
    return jnp.sum(jnp.where(same, line, 0.0), axis=1, keepdims=True)


def kernel(
    devices,
    most,
    scale,
    lengths_hbm,
    named_hbm,
    slot_hbm,
    text_lengths_hbm,
    queries_hbm,
    image_keys_hbm,
    image_values_hbm,
    text_keys_hbm,
    text_values_hbm,
    out_ref,
    lengths_ref,
    named_ref,
    slot_ref,
    text_lengths_ref,
    queries,
    keys,
    values,
    text_keys,
    text_values,
    bias,
    pick,
    asked,
    incoming,
    answer,
    answer_lse,
    back,
    back_lse,
    text_out,
    shares,
    text_lse,
    far_sem,
    first_sem,
    load_sem,
    text_sem,
    ask_send,
    ask_recv,
    out_send,
    out_recv,
    lse_send,
    lse_recv,
):
    held, local_kv, tokens, size = image_keys_hbm.shape
    heads, rows, _ = queries_hbm.shape
    text_tokens = text_keys_hbm.shape[2]
    images = slot_hbm.shape[1]
    slots = held * most
    group = heads // local_kv
    me = lax.axis_index("seq")
    others = devices - 1

    reach = devices // 4
    close = 2 * reach
    stages = [(0, 2)]
    while stages[-1][1] < reach:
        stages.append((stages[-1][1], 2 * stages[-1][1]))

    def ring(at):
        spot_at = me + at
        return spot_at - (spot_at >= devices) * devices

    def both(hops, step):
        return hops + (step % 2) * (devices - 2 * hops)

    def near_place(step):
        turn = step // 2
        hops, before = -turn, 0
        for low, high in stages:
            hops = hops + (turn >= low) * (low + high - before)
            before = low + high
        return both(hops, step)

    def far_place(step):
        hops = devices // 2 - (step + 1) // 2
        return hops + (1 - step % 2) * (devices - 2 * hops)

    def ask(at):
        return pltpu.make_async_remote_copy(
            src_ref=asked.at[at],
            dst_ref=incoming.at[at],
            send_sem=ask_send.at[at],
            recv_sem=ask_recv.at[at],
            device_id={"seq": ring(at)},
            device_id_type=MESH,
        )

    def reply(at):
        return pltpu.make_async_remote_copy(
            src_ref=answer.at[at],
            dst_ref=back.at[at],
            send_sem=out_send.at[at],
            recv_sem=out_recv.at[at],
            device_id={"seq": ring(devices - at)},
            device_id_type=MESH,
        )

    def reply_lse(at):
        return pltpu.make_async_remote_copy(
            src_ref=answer_lse.at[at],
            dst_ref=back_lse.at[at],
            send_sem=lse_send.at[at],
            recv_sem=lse_recv.at[at],
            device_id={"seq": ring(devices - at)},
            device_id_type=MESH,
        )

    def signal(sem, hops):
        for at in (hops, devices - hops):
            pl.semaphore_signal(
                sem, inc=1, device_id={"seq": ring(at)}, device_id_type=MESH
            )

    first = [
        pltpu.make_async_copy(source, target, first_sem.at[number])
        for number, (source, target) in enumerate(
            (
                (named_hbm, named_ref),
                (slot_hbm, slot_ref),
                (queries_hbm, queries),
                (lengths_hbm, lengths_ref),
                (text_lengths_hbm, text_lengths_ref),
            )
        )
    ]
    for load in first:
        load.start()
    barrier = pltpu.get_barrier_semaphore()
    signal(barrier, 1)
    signal(barrier, 2)

    loads = []
    for image in range(held):
        for head in range(local_kv):
            for number, (source, target) in enumerate(
                ((image_keys_hbm, keys), (image_values_hbm, values))
            ):
                loads.append(
                    pltpu.make_async_copy(
                        source.at[image, head],
                        target.at[head, pl.ds(image * tokens, tokens)],
                        load_sem.at[number, image, head],
                    )
                )
    loads.append(pltpu.make_async_copy(text_keys_hbm, text_keys, text_sem.at[0]))
    loads.append(pltpu.make_async_copy(text_values_hbm, text_values, text_sem.at[1]))
    first[0].wait()
    first[1].wait()
    named = named_ref[...].astype(jnp.float32)
    slot_column = column(slot_ref[...].astype(jnp.float32))
    slot_of = jnp.where(iota((images, rows), 0) == named, slot_column, 0.0)
    slot_of = jnp.sum(slot_of, axis=0, keepdims=True)
    near = slot_of + ((devices - me) * held).astype(jnp.float32)
    near = jnp.where(near >= images, near - images, near)
    near_column = column(near)
    same = near_column == near
    earlier = iota((rows, rows), 0) < iota((rows, rows), 1)
    rank = jnp.sum(jnp.where(same & earlier, 1.0, 0.0), axis=0, keepdims=True)
    target_row = near * most + rank
    pl.semaphore_wait(barrier, 4)
    signal(far_sem.at[0], stages[0][1])
    first[2].wait()
    for load in loads:
        load.start()

    def dispatch(ranges):
        number = sum(high - low for low, high in ranges) * slots
        line = iota((number, rows), 0)
        at, shift = line, 0
        for low, high in ranges:
            at = jnp.where(line >= shift, line + (low * slots - shift), at)
            shift += (high - low) * slots
        place_in = jnp.where(at == target_row, 1.0, 0.0).astype(jnp.bfloat16)
        for head in range(heads):
            sent = jnp.dot(place_in, queries[head], preferred_element_type=jnp.float32)
            sent = sent.reshape(number // slots, slots, size).astype(jnp.bfloat16)
            start = 0
            for low, high in ranges:
                piece = sent[start : start + high - low]
                asked[low:high, head // group, pl.ds(head % group * slots, slots), :] = piece
                start += high - low

    dispatch(((0, reach + 1), (devices - reach, devices)))

    def ask_near(step, carry):
        ask(near_place(step)).start()
        return carry

    for stage, (low, high) in enumerate(stages):
        if stage > 0:
            pl.semaphore_wait(far_sem.at[stage - 1], 2)
            signal(far_sem.at[stage], high)
        lax.fori_loop(2 * low, 2 * high, ask_near, 0)

    dispatch(((reach + 1, devices - reach),))
    target = column(target_row)
    pick[...] = jnp.where(iota((rows, images * most), 1) == target, 1.0, 0.0).astype(jnp.bfloat16)
    first[3].wait()
    first[4].wait()
    row = lax.broadcasted_iota(jnp.int32, (slots, held * tokens), 0)
    token = lax.broadcasted_iota(jnp.int32, (slots, held * tokens), 1)
    valid = jnp.zeros((slots, held * tokens), jnp.bool_)
    for image in range(held):
        mine = (row >= image * most) & (row < (image + 1) * most)
        inside = (token >= image * tokens) & (token < image * tokens + lengths_ref[image])
        valid = valid | (mine & inside)
    bias[...] = jnp.where(valid, 0.0, NEGATIVE)

    for load in loads:
        load.wait()

    text_length = column(text_lengths_ref[...].astype(jnp.float32))
    text_lse[...] = jnp.broadcast_to(text_length, text_lse.shape)
    wide = CHUNK * text_tokens
    lane = lax.broadcasted_iota(jnp.int32, (CHUNK, 128), 1)

    def read_text(chunk, carry):
        start = pl.multiple_of(chunk * CHUNK, CHUNK)
        limit = text_lse[pl.ds(start, CHUNK), :][:, :1]
        ahead = iota((CHUNK, wide), 1) - iota((CHUNK, wide), 0) * text_tokens
        text_bias = jnp.where((ahead >= 0) & (ahead < limit), 0.0, NEGATIVE)
        packed = jnp.zeros((CHUNK, 128), jnp.float32)
        for kv in range(local_kv):
            asking = queries[kv * group : (kv + 1) * group, pl.ds(start, CHUNK), :]
            asking = asking.reshape(group * CHUNK, size)
            those = text_keys[pl.ds(start, CHUNK), kv].reshape(wide, size)
            scores = lax.dot_general(
                asking, those, (((1,), (1,)), ((), ())), preferred_element_type=jnp.float32
            )
            scores = scores.reshape(group, CHUNK, wide) * scale + text_bias[None]
            highest = jnp.max(scores, axis=-1, keepdims=True)
            weights = jnp.exp(scores - highest)
            total = jnp.sum(weights, axis=-1, keepdims=True)
            weights = weights.astype(jnp.bfloat16).reshape(group * CHUNK, wide)
            those = text_values[pl.ds(start, CHUNK), kv].reshape(wide, size)
            mixed = jnp.dot(weights, those, preferred_element_type=jnp.float32)
            mixed = mixed.reshape(group, CHUNK, size) / total
            text_out[kv * group : (kv + 1) * group, pl.ds(start, CHUNK), :] = mixed
            lse = highest + jnp.log(total)
            for member in range(group):
                packed = jnp.where(lane == kv * group + member, lse[member], packed)
        text_lse[pl.ds(start, CHUNK), :] = packed
        return carry

    lax.fori_loop(0, rows // CHUNK, read_text, 0)
    pl.semaphore_wait(far_sem.at[len(stages) - 1], 2)

    def ask_far(step, carry):
        ask(far_place(step)).start()
        return carry

    lax.fori_loop(0, others - close, ask_far, 0)

    spot = lax.broadcasted_iota(jnp.int32, (slots, 128), 1) - 16 * lax.broadcasted_iota(
        jnp.int32, (slots, 128), 0
    )

    def attend(read, at, out_to, lse_to):
        packed = jnp.zeros((slots, 128), jnp.float32)
        for head in range(local_kv):
            scores = lax.dot_general(
                read[at, head],
                keys[head],
                (((1,), (1,)), ((), ())),
                preferred_element_type=jnp.float32,
            )
            scores = scores.reshape(group, slots, held * tokens) * scale + bias[...][None]
            highest = jnp.max(scores, axis=-1, keepdims=True)
            weights = jnp.exp(scores - highest)
            total = jnp.sum(weights, axis=-1, keepdims=True)
            weights = weights.astype(jnp.bfloat16).reshape(group * slots, held * tokens)
            mixed = jnp.dot(weights, values[head], preferred_element_type=jnp.float32)
            mixed = mixed / total.reshape(group * slots, 1)
            out_to[at, head] = mixed.astype(jnp.bfloat16)
            lse = highest + jnp.log(total)
            for member in range(group):
                packed = jnp.where(spot == head * group + member, lse[member], packed)
        lse_to[at] = jnp.sum(packed, axis=0, keepdims=True)

    attend(asked, 0, back, back_lse)

    def serve(at):
        ask(at).wait_recv()
        attend(incoming, at, answer, answer_lse)

    def serve_near(step, carry):
        @pl.when(step > 0)
        def _():
            reply_lse(near_place(step - 1)).start()

        serve(near_place(step))
        return carry

    def serve_far(step, carry):
        @pl.when(step > 0)
        def _():
            reply(far_place(step - 1)).start()
            reply_lse(far_place(step - 1)).start()

        serve(far_place(step))
        return carry

    def send_near(step, carry):
        reply(both(reach - step // 2, step)).start()
        return carry

    lax.fori_loop(0, close, serve_near, 0)
    reply_lse(near_place(close - 1)).start()
    lax.fori_loop(0, others - close, serve_far, 0)
    reply(far_place(others - close - 1)).start()
    reply_lse(far_place(others - close - 1)).start()
    lax.fori_loop(0, close, send_near, 0)

    def settle(step, carry):
        ask(step).wait_send()
        reply_lse(step).wait()
        return carry

    def finish(step, carry):
        reply(step).wait()
        return carry

    lax.fori_loop(1, devices, settle, 0)

    target = column(target_row)
    from_at = iota((rows, devices), 1) * slots
    from_here = jnp.where((target >= from_at) & (target < from_at + slots), 1.0, 0.0)
    chosen = jnp.dot(
        from_here,
        back_lse[...].reshape(devices, 128),
        precision=lax.Precision.HIGHEST,
        preferred_element_type=jnp.float32,
    )
    offset = jnp.sum(from_here * from_at, axis=1, keepdims=True)
    start = (target - offset) * 16
    lanes = iota((rows, 128), 1)
    chosen = jnp.where((lanes >= start) & (lanes < start + 16), chosen, 0.0)
    fold = iota((128, 128), 0) - iota((128, 128), 1)
    landed = jnp.zeros((128, 128), jnp.float32)
    for line in range(slots):
        landed = jnp.where(fold == 16 * line, 1.0, landed)
    landed = jnp.where(iota((128, 128), 1) < 16, landed, 0.0)
    image_lse = jnp.dot(
        chosen, landed, precision=lax.Precision.HIGHEST, preferred_element_type=jnp.float32
    )
    top = jnp.maximum(image_lse, text_lse[...])
    image_weight = jnp.exp(image_lse - top)
    text_weight = jnp.exp(text_lse[...] - top)
    whole = image_weight + text_weight
    image_share = image_weight / whole
    text_share = text_weight / whole
    for head in range(heads):
        text_out[head] = text_out[head] * text_share[:, head : head + 1]
        shares[head] = jnp.broadcast_to(image_share[:, head : head + 1], (rows, size))

    lax.fori_loop(reach + 1, devices - reach, finish, 0)
    lax.fori_loop(1, reach + 1, finish, 0)
    lax.fori_loop(devices - reach, devices, finish, 0)
    for head in range(heads):
        came = back[:, head // group, pl.ds(head % group * slots, slots), :]
        came = came.reshape(devices * slots, size)
        image_out = jnp.dot(pick[...], came, preferred_element_type=jnp.float32)
        out_ref[head] = (shares[head] * image_out + text_out[head]).astype(jnp.bfloat16)


def on_device(
    queries,
    request_image,
    image_slot,
    image_lengths,
    image_keys,
    image_values,
    text_keys,
    text_values,
    text_lengths,
):
    rows, heads, size = queries.shape
    held, local_kv, tokens, _ = image_keys.shape
    images = image_slot.shape[0]
    devices = lax.axis_size("seq")
    most = max(2, 2 * rows // images)
    slots = held * most
    scale = 1.0 / math.sqrt(size)
    message = (devices, local_kv, heads // local_kv * slots, size)
    vmem = pl.BlockSpec(memory_space=pltpu.VMEM)
    hbm = pl.BlockSpec(memory_space=pltpu.HBM)
    links = pltpu.SemaphoreType.DMA((devices,))
    out = pl.pallas_call(
        functools.partial(kernel, devices, most, scale),
        out_shape=jax.ShapeDtypeStruct((heads, rows, size), jnp.bfloat16),
        in_specs=[hbm] * 9,
        out_specs=vmem,
        scratch_shapes=[
            pltpu.SMEM((held,), jnp.int32),
            pltpu.VMEM((1, rows), jnp.int32),
            pltpu.VMEM((1, images), jnp.int32),
            pltpu.VMEM((1, rows), jnp.int32),
            pltpu.VMEM((heads, rows, size), jnp.bfloat16),
            pltpu.VMEM((local_kv, held * tokens, size), jnp.bfloat16),
            pltpu.VMEM((local_kv, held * tokens, size), jnp.bfloat16),
            pltpu.VMEM(text_keys.shape, jnp.bfloat16),
            pltpu.VMEM(text_values.shape, jnp.bfloat16),
            pltpu.VMEM((slots, held * tokens), jnp.float32),
            pltpu.VMEM((rows, images * most), jnp.bfloat16),
            pltpu.VMEM(message, jnp.bfloat16),
            pltpu.VMEM(message, jnp.bfloat16),
            pltpu.VMEM(message, jnp.bfloat16),
            pltpu.VMEM((devices, 1, 128), jnp.float32),
            pltpu.VMEM(message, jnp.bfloat16),
            pltpu.VMEM((devices, 1, 128), jnp.float32),
            pltpu.VMEM((heads, rows, size), jnp.float32),
            pltpu.VMEM((heads, rows, size), jnp.float32),
            pltpu.VMEM((rows, 128), jnp.float32),
            pltpu.SemaphoreType.REGULAR((8,)),
            pltpu.SemaphoreType.DMA((5,)),
            pltpu.SemaphoreType.DMA((2, held, local_kv)),
            pltpu.SemaphoreType.DMA((2,)),
            links,
            links,
            links,
            links,
            links,
            links,
        ],
        compiler_params=pltpu.CompilerParams(
            collective_id=0, has_side_effects=True, vmem_limit_bytes=32 * 1024 * 1024
        ),
    )(
        *(
            pltpu.with_memory_space_constraint(array, pltpu.HBM)
            for array in (
                image_lengths,
                request_image.reshape(1, rows),
                image_slot.reshape(1, images),
                text_lengths.reshape(1, rows),
                queries.transpose(1, 0, 2),
                image_keys,
                image_values,
                text_keys,
                text_values,
            )
        )
    )
    return out.transpose(1, 0, 2)


def solution(mesh):
    in_specs = (
        P(("groups", "seq"), "head", None),
        P(("groups", "seq"), None),
        P("groups"),
        P(("groups", "seq")),
        P(("groups", "seq"), "head", None, None),
        P(("groups", "seq"), "head", None, None),
        P(("groups", "seq"), "head", None, None),
        P(("groups", "seq"), "head", None, None),
        P(("groups", "seq")),
    )
    out_specs = P(("groups", "seq"), "head", None)
    return jax.shard_map(
        on_device, mesh=mesh, in_specs=in_specs, out_specs=out_specs, check_vma=False
    )
```
